32 devices in a mesh: gz: 4 (over y, core), tile: 8 (over z, x).
Axes of the slice: x: 2, y: 2, z: 4, core: 2. Of those that a mesh axis runs over, the one named last changes fastest.
Arguments:
- density: bfloat16 [32, 64, 512], P('gz', 'tile'), may hold values from -6 to 6
- w_first: bfloat16 [8, 1, 3, 3, 3], replicated, may hold values from -1.75 to 1.75
- b_first: float32 [8], replicated, may hold values from -1.25 to 1.25
- w_second: bfloat16 [8, 8, 3, 3, 3], replicated, may hold values from -0.5 to 0.5
- b_second: float32 [8], replicated, may hold values from -1.25 to 1.25
- w_third: bfloat16 [16, 8, 3, 3, 3], replicated, may hold values from -0.5 to 0.5
- b_third: float32 [16], replicated, may hold values from -1.25 to 1.25
- w_fourth: bfloat16 [16, 16, 3, 3, 3], replicated, may hold values from -0.4375 to 0.4375
- b_fourth: float32 [16], replicated, may hold values from -1.25 to 1.25
- w_fifth: bfloat16 [8, 24, 3, 3, 3], replicated, may hold values from -0.3125 to 0.3125
- b_fifth: float32 [8], replicated, may hold values from -1.25 to 1.25
- w_sixth: bfloat16 [8, 8, 3, 3, 3], replicated, may hold values from -0.5 to 0.5
- b_sixth: float32 [8], replicated, may hold values from -1.25 to 1.25
- w_head: bfloat16 [8], replicated, may hold values from -3 to 3
- b_head: float32 [1], replicated, may hold values from -1.75 to 1.75
Outputs:
- field: float32 [32, 64, 512], P('gz', 'tile')
The draws below stay inside these ranges and needn't reach their ends.
All inputs are finite; a program needn't handle non-finite values.
Results may differ from the reference program's by a relative error of at most 0.012.
Values may be sent and summed in bfloat16 or wider, within the bound.
No kernel may reach another device: no remote copies, remote signals or barrier semaphores. Data moves between devices by JAX's collectives and lax.ppermute only.
A program may use at most 128 MiB of HBM per device.

```python
import jax
import jax.numpy as jnp
from jax import lax

CF = 8
CC = 16
NY = 512
CJ = 24
NZ = 32
NX = 64


def block_levels(rng, shape, shards, low, top_value):
    level, own = 1.0, jax.random.fold_in(rng, 6)
    for dim, blocks in shards:
        heights = jnp.exp(jax.random.uniform(jax.random.fold_in(own, dim), (blocks,), jnp.float32, low / len(shards), top_value / len(shards)))
        level = level * jnp.repeat(heights, shape[dim] // blocks).reshape([-1 if axis == dim else 1 for axis in range(len(shape))])
    return level


def noise(own_key, extent, spread, limit, split=(), dtype=jnp.bfloat16):
    drawn = jax.random.normal(own_key, extent, jnp.float32) * spread
    if len(split) > 0:
        drawn = block_levels(own_key, extent, split, -0.22, 0.18) * drawn
    return jnp.clip(drawn, min=-limit, max=limit).astype(dtype)


def setup_inputs(seed: int = 0) -> dict:
    key_of = jax.random.split(jax.random.key(seed), 16)
    return {
        "density": noise(key_of[0], (NZ, NX, NY), 1.0, 6.0, ((0, 4), (1, 8))),
        "w_first": noise(key_of[1], (CF, 1, 3, 3, 3), 0.27, 1.75),
        "b_first": noise(key_of[2], (CF,), 0.2, 1.25, (), jnp.float32),
        "w_second": noise(key_of[3], (CF, CF, 3, 3, 3), 0.096, 0.5),
        "b_second": noise(key_of[4], (CF,), 0.2, 1.25, (), jnp.float32),
        "w_third": noise(key_of[5], (CC, CF, 3, 3, 3), 0.096, 0.5),
        "b_third": noise(key_of[6], (CC,), 0.2, 1.25, (), jnp.float32),
        "w_fourth": noise(key_of[7], (CC, CC, 3, 3, 3), 0.068, 0.4375),
        "b_fourth": noise(key_of[8], (CC,), 0.2, 1.25, (), jnp.float32),
        "w_fifth": noise(key_of[9], (CF, CJ, 3, 3, 3), 0.056, 0.3125),
        "b_fifth": noise(key_of[10], (CF,), 0.2, 1.25, (), jnp.float32),
        "w_sixth": noise(key_of[11], (CF, CF, 3, 3, 3), 0.096, 0.5),
        "b_sixth": noise(key_of[12], (CF,), 0.2, 1.25, (), jnp.float32),
        "w_head": noise(key_of[13], (CF,), 0.5, 3.0),
        "b_head": noise(key_of[14], (1,), 0.3, 1.75, (), jnp.float32),
    }


def convolve(values, weight, bias):
    padded = jnp.pad(values, ((0, 0), (1, 1), (1, 1), (1, 1)), mode="wrap")
    out = lax.conv_general_dilated(padded[None].astype(jnp.float32), weight.astype(jnp.float32), (1, 1, 1), "VALID", dimension_numbers=("NCDHW", "OIDHW", "NCDHW"), precision=lax.Precision.HIGHEST)[0]
    out = out + bias[:, None, None, None]
    return jnp.maximum(out, 0.1 * out).astype(jnp.bfloat16)


def reference(density, w_first, b_first, w_second, b_second, w_third, b_third, w_fourth, b_fourth, w_fifth, b_fifth, w_sixth, b_sixth, w_head, b_head):
    first = convolve(density[None], w_first, b_first)
    skip = convolve(first, w_second, b_second)
    chans, zlen, xlen, ylen = skip.shape
    pooled = skip.astype(jnp.float32).reshape(chans, zlen // 2, 2, xlen // 2, 2, ylen // 2, 2).mean(axis=(2, 4, 6)).astype(jnp.bfloat16)
    coarse_one = convolve(pooled, w_third, b_third)
    coarse_two = convolve(coarse_one, w_fourth, b_fourth)
    upsampled = jnp.repeat(jnp.repeat(jnp.repeat(coarse_two, 2, axis=1), 2, axis=2), 2, axis=3)
    joined = jnp.concatenate([skip, upsampled], axis=0)
    decoded = convolve(joined, w_fifth, b_fifth)
    refined = convolve(decoded, w_sixth, b_sixth)
    return jnp.einsum("c,czxy->zxy", w_head.astype(jnp.float32), refined.astype(jnp.float32), precision=lax.Precision.HIGHEST) + b_head[0]
```

```python
import numpy as np
import jax
import jax.numpy as jnp
from jax import lax
from jax.experimental import pallas as pl
from jax.experimental.pallas import tpu as pltpu
from jax.sharding import PartitionSpec as P

BF = jnp.bfloat16
F32 = jnp.float32
HALO = 8
GROUP = 8
GROUP5 = 6


def up(n, m):
    return -(-n // m) * m


def starts(total, size):
    size = min(size, total)
    s = list(range(0, total - size + 1, size))
    if s[-1] + size < total:
        s.append(total - size)
    return size, s


def lanes_of(dims, row_of, rows2_of, x_of, width):
    zs, xs, cs = dims
    t = np.full((3, width), -1, np.int32)
    for z in range(zs):
        for x in range(xs):
            for i in range(cs):
                c = (z * xs + x) * cs + i
                t[0, c] = row_of(z, x, i)
                t[1, c] = rows2_of(z, x, i)
                t[2, c] = x_of(z, x, i)
    return t


class Plan:
    def __init__(self, zl, xl, ny, cf, cc):
        h = HALO
        self.zl, self.xl, self.ny, self.cf, self.cc = zl, xl, ny, cf, cc
        self.nh = ny // 2
        self.zd, self.xd = zl + 2 * h, xl + 2 * h
        self.z1, self.x1 = self.zd - 2, self.xd - 2
        self.z2, self.x2 = self.zd - 4, self.xd - 4
        self.zp, self.xp = self.z2 // 2, self.x2 // 2
        self.z3, self.x3 = self.zp - 2, self.xp - 2
        self.z4, self.x4 = self.zp - 4, self.xp - 4
        self.zs, self.xs = zl + 4, xl + 4
        self.z5, self.x5 = zl + 2, xl + 2
        self.sx = up(3 * self.xd, 16)
        self.k1 = up(3 * self.sx, 128)
        self.g2, self.s2 = starts(self.x2, GROUP)
        self.g5, self.s5 = starts(self.x5, GROUP5)
        self.g6 = self.xl
        self.k2 = up(3 * (self.g2 + 2) * cf, 128)
        self.k3 = up(3 * self.xp * cf, 128)
        self.k4 = up(3 * self.x3 * cc, 128)
        self.k5 = up(3 * (self.g5 + 2) * cf, 128)
        self.kc = up(2 * self.x4 * cc, 128)
        self.k6 = up(3 * self.x5 * cf, 128)
        self.cells = zl * xl

    def tables(self):
        cf, cc = self.cf, self.cc
        n = 3 * cf + cc
        none = lambda z, x, i: -1
        xof = lambda z, x, i: x
        a2 = lanes_of((3, self.g2 + 2, cf), lambda z, x, i: z * n + i, none, xof, self.k2)
        a6 = lanes_of((3, self.x5, cf), lambda z, x, i: z * n + cf + i, none, xof, self.k6)
        a5 = lanes_of((3, self.g5 + 2, cf), lambda z, x, i: z * n + 2 * cf + i, none, xof, self.k5)
        o = 3 * cf
        ce = lanes_of(
            (2, self.x4, cc),
            lambda z, x, i: z * n + o + i,
            lambda z, x, i: 2 * n + o + i if z == 1 else -1,
            xof,
            self.kc,
        )
        co = lanes_of(
            (2, self.x4, cc),
            lambda z, x, i: 2 * z * n + o + i,
            lambda z, x, i: n + o + i if z == 0 else -1,
            xof,
            self.kc,
        )
        m = cf + cc
        b3 = lanes_of((3, self.xp, cf), lambda z, x, i: z * m + i, none, xof, self.k3)
        b4 = lanes_of((3, self.x3, cc), lambda z, x, i: z * m + cf + i, none, xof, self.k4)
        f1 = np.full((3, self.k1), -1, np.int32)
        for z in range(3):
            for dy in range(3):
                for x in range(self.xd):
                    c = z * self.sx + dy * self.xd + x
                    f1[0, c] = z * 3 + dy
                    f1[2, c] = x
        return [a2, a6, a5, ce, co, b3, b4, f1]


def prep_kernel(plan, widths, tab, wa, wb, w1, wh, a1, a2, a3, a4, a5, ac0, ac1, a6, hd, pm, pt):
    p = plan
    cf, cc = p.cf, p.cc
    off = np.concatenate([[0], np.cumsum(widths)]).tolist()

    def one_hot(i, j, rows):
        lo, hi = off[i], off[j]
        r = lax.broadcasted_iota(jnp.int32, (rows, hi - lo), 0)
        m = (r == tab[0:1, lo:hi]) | (r == tab[1:2, lo:hi])
        return jnp.where(m, 1.0, 0.0).astype(BF)

    def band(g, base, width, i, pick, outs, co, out_ref, dys):
        xi = tab[2:3, off[i] : off[i] + width]
        parts = []
        for dy in range(dys):
            for xo in range(outs):
                acc = jnp.zeros((co, width), F32)
                for dx in range(3):
                    r = (dx * dys + dy) * co
                    acc = acc + jnp.where(
                        xi == pick(xo, dx), g[r : r + co, base : base + width], 0.0
                    )
                parts.append(acc)
        out_ref[...] = jnp.concatenate(parts, axis=0).astype(BF)

    near = lambda xo, dx: xo + dx
    half = lambda xo, dx: (xo + dx) // 2
    ga = jnp.dot(wa[...], one_hot(0, 5, wa.shape[1]), preferred_element_type=F32)
    gb = jnp.dot(wb[...], one_hot(5, 7, wb.shape[1]), preferred_element_type=F32)
    g1 = jnp.dot(w1[...], one_hot(7, 8, w1.shape[1]), preferred_element_type=F32)
    band(g1, 0, p.k1, 7, near, p.x1, cf, a1, 1)
    band(ga, off[0], p.k2, 0, near, p.g2, cf, a2, 3)
    band(ga, off[1], p.k6, 1, near, p.xl, cf, a6, 3)
    band(ga, off[2], p.k5, 2, near, p.g5, cf, a5, 3)
    band(ga, off[3], p.kc, 3, half, p.x5, cf, ac0, 3)
    band(ga, off[4], p.kc, 4, half, p.x5, cf, ac1, 3)
    band(gb, 0, p.k3, 5, near, p.x3, cc, a3, 3)
    band(gb, p.k3, p.k4, 6, near, p.x4, cc, a4, 3)
    r = lax.broadcasted_iota(jnp.int32, (p.cells, p.cells * cf), 0)
    c = lax.broadcasted_iota(jnp.int32, (p.cells, p.cells * cf), 1)
    d = c - r * cf
    hd[...] = jnp.where((d >= 0) & (d < cf), wh[...], 0.0).astype(BF)
    r = lax.broadcasted_iota(jnp.int32, (p.ny, p.ny), 0)
    c = lax.broadcasted_iota(jnp.int32, (p.ny, p.ny), 1)
    fold = lambda k: jnp.where(k < p.nh, 2 * k, 2 * (k - p.nh) + 1)
    pm[...] = jnp.where(r == fold(c), 1.0, 0.0).astype(BF)
    pt[...] = jnp.where(c == fold(r), 1.0, 0.0).astype(BF)


def repeat(n, unroll, body):
    unroll = max(u for u in range(1, unroll + 1) if n % u == 0)
    if unroll == n:
        for k in range(n):
            body(k)
        return

    def step(t, carry):
        for k in range(unroll):
            body(t * unroll + k)
        return carry

    lax.fori_loop(0, n // unroll, step, 0)


def main_kernel(plan, *refs):
    p = plan
    blocks = refs[:9]
    (a1, a2, a3, a4, a5, ac0, ac1, a6, hd, pm, pt, bias, out) = refs[9:22]
    (dd, se, so, m1, sk, po, c1, c2, de, rf) = refs[22:]
    cf, cc, nh = p.cf, p.cc, p.nh
    b_first, b_second, b_third, b_fourth, b_fifth, b_sixth = (
        bias[lo:hi, :]
        for lo, hi in np.array(
            [
                (0, cf),
                (cf, 2 * cf),
                (2 * cf, 2 * cf + cc),
                (2 * cf + cc, 2 * cf + 2 * cc),
                (2 * cf + 2 * cc, 3 * cf + 2 * cc),
                (3 * cf + 2 * cc, 4 * cf + 2 * cc),
            ]
        ).tolist()
    )

    def dot(a, b):
        return jnp.dot(a, b, preferred_element_type=F32)

    def act(v, b, c):
        n = v.shape[0] // c
        u = v.reshape(n, c, nh) + b[None]
        return jnp.maximum(u, 0.1 * u).reshape(n * c, nh).astype(BF)

    def right(v):
        return pltpu.roll(v, 1, 1)

    def left(v):
        return pltpu.roll(v, nh - 1, 1)

    def window(ref, base, slab, rows, k, lo):
        parts = [
            ref[pl.ds(pl.multiple_of(base + dz * slab, 16), rows), lo : lo + nh] for dz in range(3)
        ]
        fill = k - 3 * rows
        while fill > 0:
            parts.append(parts[0][: min(fill, rows)])
            fill -= rows
        return jnp.concatenate(parts, axis=0)

    def taps(e, o, n):
        even = right(o[:n]) + e[n : 2 * n] + o[2 * n :]
        odd = e[:n] + o[n : 2 * n] + left(e[2 * n :])
        return even, odd

    h = HALO
    stacked = jnp.concatenate([b[...] for b in blocks], axis=0)
    split = dot(stacked, pm[...])
    row = 0
    for bz, nz in ((0, h), (h, p.zl), (h + p.zl, h)):
        for bx, nx in ((0, h), (h, p.xl), (h + p.xl, h)):
            dd[bz : bz + nz, bx : bx + nx, :] = split[row : row + nz * nx].reshape(nz, nx, p.ny)
            row += nz * nx

    def stack(z):
        e = dd[z, :, :nh]
        o = dd[z, :, nh:]
        pad = jnp.zeros((p.sx - 3 * p.xd, nh), F32)
        at = pl.ds(pl.multiple_of(z * p.sx, 16), p.sx)
        se[at, :] = jnp.concatenate([right(o), e, o, pad], axis=0).astype(BF)
        so[at, :] = jnp.concatenate([e, o, left(e), pad], axis=0).astype(BF)

    repeat(p.zd, 6, stack)
    tail = p.zd * p.sx
    se[tail:, :] = jnp.zeros((se.shape[0] - tail, nh), BF)
    so[tail:, :] = jnp.zeros((so.shape[0] - tail, nh), BF)

    r1 = p.x1 * cf

    def first(z):
        at = pl.ds(pl.multiple_of(z * p.sx, 16), p.k1)
        to = pl.ds(pl.multiple_of(z * r1, 16), r1)
        m1[to, :nh] = act(dot(a1[...], se[at, :]), b_first, cf)
        m1[to, nh:] = act(dot(a1[...], so[at, :]), b_first, cf)

    repeat(p.z1, 2, first)

    rp = p.xp * cf
    rs = p.xs * cf
    lead = (p.x2 - p.xs) // 2

    def second(zz):
        done = 0
        for s in p.s2:
            n = p.g2 * cf
            total = None
            skip = s + p.g2 - done
            new = (done - s) * cf
            for dz in range(2):
                base = (2 * zz + dz) * r1 + s * cf
                rows = (p.g2 + 2) * cf
                e = dot(a2[...], window(m1, base, r1, rows, p.k2, 0))
                o = dot(a2[...], window(m1, base, r1, rows, p.k2, nh))
                even, odd = taps(e, o, n)
                even = act(even[new:], b_second, cf)
                odd = act(odd[new:], b_second, cf)
                lo, hi = max(done, lead), min(s + p.g2, lead + p.xs)
                if lo < hi:
                    src = slice((lo - done) * cf, (hi - done) * cf)
                    to = pl.ds(
                        pl.multiple_of((2 * zz + dz) * rs + (lo - lead) * cf, 16), (hi - lo) * cf
                    )
                    sk[to, :nh] = even[src]
                    sk[to, nh:] = odd[src]
                t = even.astype(F32) + odd.astype(F32)
                t = t.reshape(skip // 2, 2, cf, nh)
                t = t[:, 0] + t[:, 1]
                total = t if total is None else total + t
            pooled = (0.125 * total).reshape(skip // 2 * cf, nh).astype(BF)
            po[pl.ds(pl.multiple_of(zz * rp + done // 2 * cf, 16), skip // 2 * cf), :] = pooled
            done = s + p.g2

    repeat(p.zp, 1, second)
    tail = p.zp * rp
    po[tail:, :] = jnp.zeros((po.shape[0] - tail, nh), BF)

    r3 = p.x3 * cc

    def third(z):
        v = dot(a3[...], po[pl.ds(pl.multiple_of(z * rp, 16), p.k3), :])
        v = right(v[:r3]) + v[r3 : 2 * r3] + left(v[2 * r3 :])
        c1[pl.ds(pl.multiple_of(z * r3, 16), r3), :] = act(v, b_third, cc)

    repeat(p.z3, 4, third)
    r4 = p.x4 * cc

    def fourth(z):
        v = dot(a4[...], window(c1, z * r3, r3, r3, p.k4, 0))
        v = right(v[:r4]) + v[r4 : 2 * r4] + left(v[2 * r4 :])
        c2[pl.ds(pl.multiple_of(z * r4, 16), r4), :] = act(v, b_fourth, cc)

    repeat(p.z4, 6, fourth)
    tail = p.z4 * r4
    c2[tail:, :] = jnp.zeros((c2.shape[0] - tail, nh), BF)
    r5 = p.x5 * cf
    skip_lead = (p.z2 - p.zs) // 2

    def fifth(pair):
        for odd_z in range(2):
            z = 2 * pair + odd_z
            ac = ac0 if odd_z else ac1
            q = dot(ac[...], c2[pl.ds(pl.multiple_of(pair * r4, 16), p.kc), :])
            q0, q1, q2 = q[:r5], q[r5 : 2 * r5], q[2 * r5 :]
            done = 0
            e3 = [[], [], []]
            o3 = [[], [], []]
            n = p.g5 * cf
            for s in p.s5:
                rows = (p.g5 + 2) * cf
                base = (z + skip_lead) * rs + s * cf
                e = dot(a5[...], window(sk, base, rs, rows, p.k5, 0))
                o = dot(a5[...], window(sk, base, rs, rows, p.k5, nh))
                new = (done - s) * cf
                for dy in range(3):
                    e3[dy].append(e[dy * n + new : (dy + 1) * n])
                    o3[dy].append(o[dy * n + new : (dy + 1) * n])
                done = s + p.g5
            e0, e1, e2 = (jnp.concatenate(v, axis=0) for v in e3)
            o0, o1, o2 = (jnp.concatenate(v, axis=0) for v in o3)
            even = right(o0 + q0) + (e1 + o2 + (q1 + q2))
            odd = (e0 + o1 + (q0 + q1)) + left(e2 + q2)
            to = pl.ds(pl.multiple_of(z * r5, 16), r5)
            de[to, :nh] = act(even, b_fifth, cf)
            de[to, nh:] = act(odd, b_fifth, cf)

    repeat(p.z5 // 2, 1, fifth)
    tail = p.z5 * r5
    de[tail:, :] = jnp.zeros((de.shape[0] - tail, p.ny), BF)
    r6 = p.xl * cf

    def sixth(z):
        at = pl.ds(pl.multiple_of(z * r5, 16), p.k6)
        e = dot(a6[...], de[at, :nh])
        o = dot(a6[...], de[at, nh:])
        even, odd = taps(e, o, r6)
        to = pl.ds(pl.multiple_of(z * r6, 16), r6)
        rf[to, :nh] = act(even, b_sixth, cf)
        rf[to, nh:] = act(odd, b_sixth, cf)

    repeat(p.zl, 4, sixth)
    last = 4 * cf + 2 * cc
    field = dot(hd[...], rf[...]) + bias[last : last + 1, 0:1]
    high = field.astype(BF)
    low = (field - high.astype(F32)).astype(BF)
    both = dot(jnp.concatenate([high, low], axis=0), pt[...])
    out[...] = both[: p.cells] + both[p.cells :]


def shift(block, axis, step):
    count = lax.axis_size(axis)
    return lax.ppermute(block, axis, [((i + step) % count, i) for i in range(count)])


def body(
    density,
    w_first,
    b_first,
    w_second,
    b_second,
    w_third,
    b_third,
    w_fourth,
    b_fourth,
    w_fifth,
    b_fifth,
    w_sixth,
    b_sixth,
    w_head,
    b_head,
):
    zl, xl, ny = density.shape
    cf, cc = w_second.shape[0], w_third.shape[0]
    h = HALO
    p = Plan(zl, xl, ny, cf, cc)

    left = shift(density[:, xl - h :], "tile", -1)
    right = shift(density[:, :h], "tile", 1)
    columns = [left, density, right]
    below = [shift(c[zl - h :], "gz", -1) for c in columns]
    above = [shift(c[:h], "gz", 1) for c in columns]
    blocks = [b.reshape(-1, ny) for b in below + columns + above]

    def table(w):
        return w.transpose(3, 4, 0, 2, 1).reshape(9 * w.shape[0], 3 * w.shape[1])

    wa = table(jnp.concatenate([w_second, w_sixth, w_fifth], axis=1))
    wb = table(jnp.concatenate([w_third, w_fourth], axis=1))
    w1 = w_first[:, 0].transpose(2, 0, 1, 3).reshape(3 * cf, 9)
    wh = jnp.tile(w_head.astype(F32), p.cells)[None]
    tabs = p.tables()
    widths = [t.shape[1] for t in tabs]
    tab = jnp.asarray(np.concatenate(tabs, axis=1))
    biases = jnp.concatenate(
        [b_first, b_second, b_third, b_fourth, b_fifth, b_sixth, jnp.tile(b_head, 8)]
    )
    bias = jnp.broadcast_to(biases[:, None], (biases.shape[0], p.nh))

    sds = jax.ShapeDtypeStruct
    mats = [
        sds((p.x1 * cf, p.k1), BF),
        sds((3 * p.g2 * cf, p.k2), BF),
        sds((3 * p.x3 * cc, p.k3), BF),
        sds((3 * p.x4 * cc, p.k4), BF),
        sds((3 * p.g5 * cf, p.k5), BF),
        sds((3 * p.x5 * cf, p.kc), BF),
        sds((3 * p.x5 * cf, p.kc), BF),
        sds((3 * p.xl * cf, p.k6), BF),
        sds((p.cells, p.cells * cf), BF),
        sds((ny, ny), BF),
        sds((ny, ny), BF),
    ]
    vmem = pl.BlockSpec(memory_space=pltpu.VMEM)
    tables = pl.pallas_call(
        lambda *refs: prep_kernel(p, widths, *refs),
        in_specs=[vmem] * 5,
        out_specs=[vmem] * len(mats),
        out_shape=mats,
        name="bands",
    )(tab, wa, wb, w1, wh)

    field = pl.pallas_call(
        lambda *refs: main_kernel(p, *refs),
        in_specs=[vmem] * (9 + len(mats) + 1),
        out_specs=vmem,
        out_shape=sds((p.cells, ny), F32),
        scratch_shapes=[
            pltpu.VMEM((p.zd, p.xd, ny), F32),
            pltpu.VMEM((p.zd * p.sx + 256, p.nh), BF),
            pltpu.VMEM((p.zd * p.sx + 256, p.nh), BF),
            pltpu.VMEM((p.z1 * p.x1 * cf, ny), BF),
            pltpu.VMEM((p.z2 * p.xs * cf, ny), BF),
            pltpu.VMEM((p.zp * p.xp * cf + 256, p.nh), BF),
            pltpu.VMEM((p.z3 * p.x3 * cc, p.nh), BF),
            pltpu.VMEM((p.z4 * p.x4 * cc + 256, p.nh), BF),
            pltpu.VMEM((p.z5 * p.x5 * cf + 256, ny), BF),
            pltpu.VMEM((p.cells * cf, ny), BF),
        ],
        name="unet",
    )(*blocks, *tables, bias)
    return field.reshape(zl, xl, ny)


def solution(mesh):
    return jax.shard_map(
        body,
        mesh=mesh,
        in_specs=(P("gz", "tile", None),) + (P(),) * 14,
        out_specs=P("gz", "tile", None),
        check_vma=False,
    )
```

```python
import numpy as np
import jax
import jax.numpy as jnp
from jax import lax
from jax.experimental import pallas as pl
from jax.experimental.pallas import tpu as pltpu
from jax.sharding import PartitionSpec as P


BF = jnp.bfloat16
F32 = jnp.float32
HALO = 8
GROUP = 8
GROUP5 = 6
LANES = 128
U_STACK, U_FIRST, U_SECOND, U_THIRD, U_FOURTH, U_FIFTH, U_SIXTH = 6, 11, 2, 8, 6, 5, 8
MATS = 13
ORDER = (10, 12, 0, 1, 2, 3, 4, 5, 6, 7, 8, 9, 11)
CODE = 64


def up(n, m):
    return -(-n // m) * m


def starts(total, size):
    size = min(size, total)
    s = list(range(0, total - size + 1, size))
    if s[-1] + size < total:
        s.append(total - size)
    return size, s


def lanes_of(dims, row_of, rows2_of, x_of, width):
    zs, xs, cs = dims
    t = np.full((3, width), -1, np.int32)
    for z in range(zs):
        for x in range(xs):
            for i in range(cs):
                c = (z * xs + x) * cs + i
                t[0, c] = row_of(z, x, i)
                t[1, c] = rows2_of(z, x, i)
                t[2, c] = x_of(z, x, i)
    return t


class Plan:
    def __init__(self, zl, xl, ny, cf, cc):
        h = HALO
        self.zl, self.xl, self.ny, self.cf, self.cc = zl, xl, ny, cf, cc
        self.nh = ny // 2
        self.zd, self.xd = zl + 2 * h, xl + 2 * h
        self.z1, self.x1 = self.zd - 2, self.xd - 2
        self.z2, self.x2 = self.zd - 4, self.xd - 4
        self.zp, self.xp = self.z2 // 2, self.x2 // 2
        self.z3, self.x3 = self.zp - 2, self.xp - 2
        self.z4, self.x4 = self.zp - 4, self.xp - 4
        self.zs, self.xs = zl + 4, xl + 4
        self.z5, self.x5 = zl + 2, xl + 2
        self.sx = up(3 * self.xd, 16)
        self.k1 = up(3 * self.sx, 128)
        self.n2 = self.x2 // GROUP
        self.rest = self.x2 - self.n2 * GROUP
        self.g5, self.s5 = starts(self.x5, GROUP5)
        self.k2 = up(3 * (GROUP + 2) * cf, 128)
        self.kr = up(4 * (self.rest + 2) * cf, 128)
        self.k3 = up(3 * self.xp * cf, 128)
        self.k4 = up(3 * self.x3 * cc, 128)
        self.k5 = up(3 * (self.g5 + 2) * cf, 128)
        self.kc = up(2 * self.x4 * cc, 128)
        self.k6 = up(3 * self.x5 * cf, 128)
        self.cells = zl * xl
        self.span = 2 * LANES

    def tables(self):
        cf, cc = self.cf, self.cc
        none = lambda z, x, i: -1
        xof = lambda z, x, i: x
        code = lambda z, x, i: CODE * z + i
        a2 = lanes_of((3, GROUP + 2, cf), code, none, xof, self.k2)
        r0 = lanes_of((4, self.rest + 2, cf), lambda z, x, i: CODE * z + i if z < 3 else -1, none, xof, self.kr)
        r1 = lanes_of((4, self.rest + 2, cf), lambda z, x, i: CODE * (z - 1) + i if z else -1, none, xof, self.kr)
        a6 = lanes_of((3, self.x5, cf), code, none, xof, self.k6)
        a5 = lanes_of((3, self.g5 + 2, cf), code, none, xof, self.k5)
        ce = lanes_of(
            (2, self.x4, cc),
            lambda z, x, i: CODE * z + cf + i,
            lambda z, x, i: CODE * 2 + cf + i if z == 1 else -1,
            xof,
            self.kc,
        )
        co = lanes_of(
            (2, self.x4, cc),
            lambda z, x, i: CODE * 2 * z + cf + i,
            lambda z, x, i: CODE + cf + i if z == 0 else -1,
            xof,
            self.kc,
        )
        b4 = lanes_of((3, self.x3, cc), code, none, xof, self.k4)
        b3 = lanes_of((3, self.xp, cf), lambda z, x, i: 9 * cf * z + i, none, xof, self.k3)
        f1 = np.full((3, self.k1), -1, np.int32)
        for z in range(3):
            for dy in range(3):
                for x in range(self.xd):
                    c = z * self.sx + dy * self.xd + x
                    f1[0, c] = z * 24 + dy
                    f1[2, c] = x
        hd = lanes_of((1, self.cells, cf), lambda z, x, i: i, none, xof, self.cells * cf)
        return [a2, r0, r1, a6, a5, ce, co, b4, b3, f1, hd]


def prep_kernel(plan, widths, *refs):
    (tab, w2, w6, w5, w4, w3, w1, wh) = refs[:8]
    biases = refs[8:15]
    (a1, a2, ar, a3, a4, a5, ac0, ac1, a6, hd, pm, pt, bias) = refs[15:28]
    (t1,) = refs[28:]
    p = plan
    cf, cc = p.cf, p.cc
    off = np.concatenate([[0], np.cumsum(widths)]).tolist()

    def dot(a, b):
        return jnp.dot(a, b, preferred_element_type=F32)

    def expand(w, i, j, co):
        lo, hi = off[i], off[j]
        rows = w.shape[1]
        r = lax.broadcasted_iota(jnp.int32, (rows, hi - lo), 0)
        total = None
        for dz in range(3):
            m = (r + CODE * dz == tab[0:1, lo:hi]) | (r + CODE * dz == tab[1:2, lo:hi])
            g = dot(w[dz * 9 * co : (dz + 1) * 9 * co, :], jnp.where(m, 1.0, 0.0).astype(BF))
            total = g if total is None else total + g
        return total

    def select(w, i, base):
        lo, hi = off[i], off[i + 1]
        r = lax.broadcasted_iota(jnp.int32, (w.shape[1], hi - lo), 0)
        m = (r - base == tab[0:1, lo:hi]) & (tab[0:1, lo:hi] >= 0)
        return dot(w, jnp.where(m, 1.0, 0.0).astype(BF))

    def band(pieces, i, pick, outs):
        xi = tab[2:3, off[i] : off[i + 1]]
        parts = []
        for xo in range(outs):
            acc = None
            for dx in range(3):
                v = jnp.where(xi == pick(xo, dx), pieces[dx], 0.0)
                acc = v if acc is None else acc + v
            parts.append(acc)
        return parts

    def rows_of(g, lo, width, dy, co):
        return [
            g[(dx * 3 + dy) * co : (dx * 3 + dy + 1) * co, lo : lo + width] for dx in range(3)
        ]

    def full(out, g, lo, i, pick, outs, co):
        parts = []
        for dy in range(3):
            parts += band(rows_of(g, lo, widths[i], dy, co), i, pick, outs)
        out[...] = jnp.concatenate(parts, axis=0).astype(BF)

    near = lambda xo, dx: xo + dx
    half = lambda xo, dx: (xo + dx) // 2
    t1[...] = jnp.zeros(t1.shape, F32)
    for k in range(9):
        t1[8 * k : 8 * k + 3, :cf] = w1[k // 3, k % 3].astype(F32)
    turned = t1[...].T[:cf].astype(BF)
    a1[...] = jnp.concatenate(
        band([select(turned, 9, 8 * dx) for dx in range(3)], 9, near, p.x1), axis=0
    ).astype(BF)
    g = expand(w2, 0, 3, cf)
    full(a2, g, 0, 0, near, GROUP, cf)
    parts = []
    for dy in range(3):
        for zo in range(2):
            lo = off[1 + zo]
            parts += band(rows_of(g, lo, p.kr, dy, cf), 1 + zo, near, p.rest)
    if parts:
        ar[...] = jnp.concatenate(parts, axis=0).astype(BF)
    full(a6, expand(w6, 3, 4, cf), 0, 3, near, p.xl, cf)
    g = expand(w5, 4, 7, cf)
    full(a5, g, 0, 4, near, p.g5, cf)
    full(ac0, g, off[5] - off[4], 5, half, p.x5, cf)
    full(ac1, g, off[6] - off[4], 6, half, p.x5, cf)
    full(a4, expand(w4, 7, 8, cc), 0, 7, near, p.x4, cc)
    turned = w3[...].astype(F32).T.astype(BF)
    parts = []
    for dy in range(3):
        pieces = [select(turned, 8, (3 * dx + dy) * cf) for dx in range(3)]
        parts += band(pieces, 8, near, p.x3)
    a3[...] = jnp.concatenate(parts, axis=0).astype(BF)
    v = select(jnp.broadcast_to(wh[...], (16, cf)), 10, 0)
    r = lax.broadcasted_iota(jnp.int32, (p.cells, p.cells * cf), 0)
    cell = tab[2:3, off[10] : off[11]]
    hd[...] = jnp.where(cell == r, v[0:1], 0.0).astype(BF)
    r = lax.broadcasted_iota(jnp.int32, (p.span, p.span), 0)
    c = lax.broadcasted_iota(jnp.int32, (p.span, p.span), 1)
    fold = lambda k: jnp.where(k < LANES, 2 * k, 2 * (k - LANES) + 1)
    pm[...] = jnp.where(r == fold(c), 1.0, 0.0).astype(BF)
    pt[...] = jnp.where(c == fold(r), 1.0, 0.0).astype(BF)
    at = 0
    for b in biases:
        n = b.shape[0]
        m = up(n, 8)
        r = lax.broadcasted_iota(jnp.int32, (m, p.nh), 0)
        v = jnp.zeros((m, p.nh), F32)
        for k in range(n):
            v = jnp.where(r == k, b[k], v)
        bias[at : at + m, :] = v
        at += m


def repeat(n, unroll, body):
    unroll = max(u for u in range(1, unroll + 1) if n % u == 0)
    if unroll == n:
        for k in range(n):
            body(k)
        return

    def step(t, carry):
        for k in range(unroll):
            body(t * unroll + k)
        return carry

    lax.fori_loop(0, n // unroll, step, 0)


def main_kernel(plan, *refs):
    p = plan
    n = 9 + MATS
    out = refs[n]
    (dd, se, so, m1, sk, po, c1, c2, de, rf, raw) = refs[n + 1 : n + 12]
    mats = refs[n + 12 : n + 12 + MATS]
    sem = refs[n + 12 + MATS]
    (a1, a2, ar, a3, a4, a5, ac0, ac1, a6, hd, pm, pt, bias) = mats
    copies = []
    row = 0
    for k in range(9):
        rows = refs[k].shape[0]
        copies.append(pltpu.make_async_copy(refs[k], raw.at[pl.ds(row, rows)], sem.at[k]))
        row += rows
    for k in range(MATS):
        copies.append(pltpu.make_async_copy(refs[9 + k], mats[k], sem.at[9 + k]))
    for k in list(range(9)) + [9 + ORDER[k] for k in range(MATS)]:
        copies[k].start()

    def ready(*names):
        for k in names:
            copies[k].wait()

    cf, cc, nh = p.cf, p.cc, p.nh

    def rows(lo, n):
        return bias[lo : lo + n, :]

    def dot(a, b):
        return jnp.dot(a, b, preferred_element_type=F32)

    def act(v, b, c):
        n = v.shape[0] // c
        u = v.reshape(n, c, nh) + b[None]
        return jnp.maximum(u, 0.1 * u).reshape(n * c, nh).astype(BF)

    def right(v):
        return pltpu.roll(v, 1, 1)

    def left(v):
        return pltpu.roll(v, nh - 1, 1)

    def window(ref, base, slab, rows, k, lo, slabs=3):
        parts = [
            ref[pl.ds(pl.multiple_of(base + dz * slab, 16), rows), lo : lo + nh]
            for dz in range(slabs)
        ]
        fill = k - slabs * rows
        while fill > 0:
            parts.append(parts[0][: min(fill, rows)])
            fill -= rows
        return jnp.concatenate(parts, axis=0)

    def taps(e, o, n):
        even = right(o[:n]) + e[n : 2 * n] + o[2 * n :]
        odd = e[:n] + o[n : 2 * n] + left(e[2 * n :])
        return even, odd

    h = HALO
    ready(*range(9), 9 + 10)
    span = p.span
    split = [dot(raw[:, y : y + span], pm[...]) for y in range(0, p.ny, span)]
    row = 0
    for bz, nz in ((0, h), (h, p.zl), (h + p.zl, h)):
        for bx, nx in ((0, h), (h, p.xl), (h + p.xl, h)):
            for k, v in enumerate(split):
                v = v[row : row + nz * nx].reshape(nz, nx, span)
                at = slice(k * LANES, (k + 1) * LANES)
                dd[bz : bz + nz, bx : bx + nx, at] = v[:, :, :LANES]
                at = slice(nh + k * LANES, nh + (k + 1) * LANES)
                dd[bz : bz + nz, bx : bx + nx, at] = v[:, :, LANES:]
            row += nz * nx

    def stack(z):
        e = dd[z, :, :nh]
        o = dd[z, :, nh:]
        pad = jnp.zeros((p.sx - 3 * p.xd, nh), F32)
        at = pl.ds(pl.multiple_of(z * p.sx, 16), p.sx)
        se[at, :] = jnp.concatenate([right(o), e, o, pad], axis=0).astype(BF)
        so[at, :] = jnp.concatenate([e, o, left(e), pad], axis=0).astype(BF)

    repeat(p.zd, U_STACK, stack)
    tail = p.zd * p.sx
    se[tail:, :] = jnp.zeros((se.shape[0] - tail, nh), BF)
    so[tail:, :] = jnp.zeros((so.shape[0] - tail, nh), BF)

    r1 = p.x1 * cf
    ready(9 + 0, 9 + 12)
    b_first, b_second = rows(0, cf), rows(cf, cf)
    b_third, b_fourth = rows(2 * cf, cc), rows(2 * cf + cc, cc)
    b_fifth, b_sixth = rows(2 * cf + 2 * cc, cf), rows(3 * cf + 2 * cc, cf)

    def first(z):
        at = pl.ds(pl.multiple_of(z * p.sx, 16), p.k1)
        to = pl.ds(pl.multiple_of(z * r1, 16), r1)
        m1[to, :nh] = act(dot(a1[...], se[at, :]), b_first, cf)
        m1[to, nh:] = act(dot(a1[...], so[at, :]), b_first, cf)

    repeat(p.z1, U_FIRST, first)

    rp = p.xp * cf
    rs = p.xs * cf
    lead = (p.x2 - p.xs) // 2

    ready(9 + 1, 9 + 2)

    def keep(z, s, even, odd):
        lo, hi = max(s, lead), min(s + even.shape[0] // cf, lead + p.xs)
        if lo < hi:
            src = slice((lo - s) * cf, (hi - s) * cf)
            to = pl.ds(pl.multiple_of(z * rs + (lo - lead) * cf, 16), (hi - lo) * cf)
            sk[to, :nh] = even[src]
            sk[to, nh:] = odd[src]

    def pairs(even, odd):
        t = even.astype(F32) + odd.astype(F32)
        t = t.reshape(t.shape[0] // (2 * cf), 2, cf, nh)
        return t[:, 0] + t[:, 1]

    def pool(zz, s, total):
        n = total.shape[0] * cf
        pooled = (0.125 * total).reshape(n, nh).astype(BF)
        po[pl.ds(pl.multiple_of(zz * rp + s // 2 * cf, 16), n), :] = pooled

    def second(zz):
        for s in range(0, p.n2 * GROUP, GROUP):
            n = GROUP * cf
            total = None
            for dz in range(2):
                base = (2 * zz + dz) * r1 + s * cf
                k = (GROUP + 2) * cf
                e = dot(a2[...], window(m1, base, r1, k, p.k2, 0))
                o = dot(a2[...], window(m1, base, r1, k, p.k2, nh))
                even, odd = taps(e, o, n)
                even = act(even, b_second, cf)
                odd = act(odd, b_second, cf)
                keep(2 * zz + dz, s, even, odd)
                t = pairs(even, odd)
                total = t if total is None else total + t
            pool(zz, s, total)
        if p.rest:
            s = p.n2 * GROUP
            n = p.rest * cf
            base = 2 * zz * r1 + s * cf
            k = (p.rest + 2) * cf
            e = dot(ar[...], window(m1, base, r1, k, p.kr, 0, 4))
            o = dot(ar[...], window(m1, base, r1, k, p.kr, nh, 4))
            even, odd = taps(e, o, 2 * n)
            even = act(even, b_second, cf)
            odd = act(odd, b_second, cf)
            keep(2 * zz, s, even[:n], odd[:n])
            keep(2 * zz + 1, s, even[n:], odd[n:])
            t = pairs(even, odd)
            pool(zz, s, t[: p.rest // 2] + t[p.rest // 2 :])

    repeat(p.zp, U_SECOND, second)
    tail = p.zp * rp
    po[tail:, :] = jnp.zeros((po.shape[0] - tail, nh), BF)

    r3 = p.x3 * cc

    def third(z):
        v = dot(a3[...], po[pl.ds(pl.multiple_of(z * rp, 16), p.k3), :])
        v = right(v[:r3]) + v[r3 : 2 * r3] + left(v[2 * r3 :])
        c1[pl.ds(pl.multiple_of(z * r3, 16), r3), :] = act(v, b_third, cc)

    ready(9 + 3)
    repeat(p.z3, U_THIRD, third)
    r4 = p.x4 * cc

    def fourth(z):
        v = dot(a4[...], window(c1, z * r3, r3, r3, p.k4, 0))
        v = right(v[:r4]) + v[r4 : 2 * r4] + left(v[2 * r4 :])
        c2[pl.ds(pl.multiple_of(z * r4, 16), r4), :] = act(v, b_fourth, cc)

    ready(9 + 4)
    repeat(p.z4, U_FOURTH, fourth)
    tail = p.z4 * r4
    c2[tail:, :] = jnp.zeros((c2.shape[0] - tail, nh), BF)
    r5 = p.x5 * cf
    skip_lead = (p.z2 - p.zs) // 2

    def fifth(pair):
        for odd_z in range(2):
            z = 2 * pair + odd_z
            ac = ac0 if odd_z else ac1
            q = dot(ac[...], c2[pl.ds(pl.multiple_of(pair * r4, 16), p.kc), :])
            q0, q1, q2 = q[:r5], q[r5 : 2 * r5], q[2 * r5 :]
            done = 0
            e3 = [[], [], []]
            o3 = [[], [], []]
            n = p.g5 * cf
            for s in p.s5:
                rows = (p.g5 + 2) * cf
                base = (z + skip_lead) * rs + s * cf
                e = dot(a5[...], window(sk, base, rs, rows, p.k5, 0))
                o = dot(a5[...], window(sk, base, rs, rows, p.k5, nh))
                new = (done - s) * cf
                for dy in range(3):
                    e3[dy].append(e[dy * n + new : (dy + 1) * n])
                    o3[dy].append(o[dy * n + new : (dy + 1) * n])
                done = s + p.g5
            e0, e1, e2 = (jnp.concatenate(v, axis=0) for v in e3)
            o0, o1, o2 = (jnp.concatenate(v, axis=0) for v in o3)
            even = right(o0 + q0) + (e1 + o2 + (q1 + q2))
            odd = (e0 + o1 + (q0 + q1)) + left(e2 + q2)
            to = pl.ds(pl.multiple_of(z * r5, 16), r5)
            de[to, :nh] = act(even, b_fifth, cf)
            de[to, nh:] = act(odd, b_fifth, cf)

    ready(9 + 5, 9 + 6, 9 + 7)
    repeat(p.z5 // 2, U_FIFTH, fifth)
    tail = p.z5 * r5
    de[tail:, :] = jnp.zeros((de.shape[0] - tail, p.ny), BF)
    r6 = p.xl * cf

    def sixth(z):
        at = pl.ds(pl.multiple_of(z * r5, 16), p.k6)
        e = dot(a6[...], de[at, :nh])
        o = dot(a6[...], de[at, nh:])
        even, odd = taps(e, o, r6)
        to = pl.ds(pl.multiple_of(z * r6, 16), r6)
        rf[to, :nh] = act(even, b_sixth, cf)
        rf[to, nh:] = act(odd, b_sixth, cf)

    ready(9 + 8)
    repeat(p.zl, U_SIXTH, sixth)
    last = 4 * cf + 2 * cc
    ready(9 + 9, 9 + 11)
    field = dot(hd[...], rf[...]) + bias[last : last + 1, 0:1]
    high = field.astype(BF)
    low = (field - high.astype(F32)).astype(BF)
    both = jnp.concatenate([high, low], axis=0)
    for k in range(p.ny // span):
        at = slice(k * LANES, (k + 1) * LANES)
        v = jnp.concatenate([both[:, at], both[:, nh + k * LANES : nh + (k + 1) * LANES]], axis=1)
        v = dot(v, pt[...])
        out[:, k * span : (k + 1) * span] = v[: p.cells] + v[p.cells :]


def shift(block, axis, step):
    count = lax.axis_size(axis)
    return lax.ppermute(block, axis, [((i + step) % count, i) for i in range(count)])


def body(
    density,
    w_first,
    b_first,
    w_second,
    b_second,
    w_third,
    b_third,
    w_fourth,
    b_fourth,
    w_fifth,
    b_fifth,
    w_sixth,
    b_sixth,
    w_head,
    b_head,
):
    zl, xl, ny = density.shape
    cf, cc = w_second.shape[0], w_third.shape[0]
    h = HALO
    p = Plan(zl, xl, ny, cf, cc)

    left = shift(density[:, xl - h :], "tile", -1)
    right = shift(density[:, :h], "tile", 1)
    columns = [left, density, right]
    below = [shift(c[zl - h :], "gz", -1) for c in columns]
    above = [shift(c[:h], "gz", 1) for c in columns]
    blocks = [b.reshape(-1, ny) for b in below + columns + above]

    def taps(w, *last):
        return w.transpose(2, 3, 4, *last).reshape(-1, w.shape[last[1]])

    weights = [taps(w, 0, 1) for w in (w_second, w_sixth, w_fifth, w_fourth)]
    weights += [taps(w_third, 1, 0), w_first[:, 0].transpose(1, 2, 3, 0), w_head[None]]
    biases = [b_first, b_second, b_third, b_fourth, b_fifth, b_sixth, b_head]
    tabs = p.tables()
    widths = [t.shape[1] for t in tabs]
    tab = jnp.asarray(np.concatenate(tabs, axis=1))
    bias_rows = sum(up(b.shape[0], 8) for b in biases)

    sds = jax.ShapeDtypeStruct
    mats = [
        sds((p.x1 * cf, p.k1), BF),
        sds((3 * GROUP * cf, p.k2), BF),
        sds((max(6 * p.rest * cf, 16), p.kr), BF),
        sds((3 * p.x3 * cc, p.k3), BF),
        sds((3 * p.x4 * cc, p.k4), BF),
        sds((3 * p.g5 * cf, p.k5), BF),
        sds((3 * p.x5 * cf, p.kc), BF),
        sds((3 * p.x5 * cf, p.kc), BF),
        sds((3 * p.xl * cf, p.k6), BF),
        sds((p.cells, p.cells * cf), BF),
        sds((p.span, p.span), BF),
        sds((p.span, p.span), BF),
        sds((bias_rows, p.nh), F32),
    ]
    vmem = pl.BlockSpec(memory_space=pltpu.VMEM)
    smem = pl.BlockSpec(memory_space=pltpu.SMEM)
    anym = pl.BlockSpec(memory_space=pl.ANY)
    tables = pl.pallas_call(
        lambda *refs: prep_kernel(p, widths, *refs),
        in_specs=[vmem] * 8 + [smem] * 7,
        out_specs=[vmem] * MATS,
        out_shape=mats,
        scratch_shapes=[pltpu.VMEM((72, LANES), F32)],
        name="bands",
    )(tab, *weights, *biases)

    rows = sum(b.shape[0] for b in blocks)
    field = pl.pallas_call(
        lambda *refs: main_kernel(p, *refs),
        in_specs=[anym] * (9 + MATS),
        out_specs=vmem,
        out_shape=sds((p.cells, ny), F32),
        scratch_shapes=[
            pltpu.VMEM((p.zd, p.xd, ny), F32),
            pltpu.VMEM((p.zd * p.sx + 256, p.nh), BF),
            pltpu.VMEM((p.zd * p.sx + 256, p.nh), BF),
            pltpu.VMEM((p.z1 * p.x1 * cf, ny), BF),
            pltpu.VMEM((p.z2 * p.xs * cf, ny), BF),
            pltpu.VMEM((p.zp * p.xp * cf + 256, p.nh), BF),
            pltpu.VMEM((p.z3 * p.x3 * cc, p.nh), BF),
            pltpu.VMEM((p.z4 * p.x4 * cc + 256, p.nh), BF),
            pltpu.VMEM((p.z5 * p.x5 * cf + 256, ny), BF),
            pltpu.VMEM((p.cells * cf, ny), BF),
            pltpu.VMEM((rows, ny), BF),
        ]
        + [pltpu.VMEM(m.shape, m.dtype) for m in mats]
        + [pltpu.SemaphoreType.DMA((9 + MATS,))],
        name="unet",
    )(*blocks, *tables)
    return field.reshape(zl, xl, ny)


def solution(mesh):
    return jax.shard_map(
        body,
        mesh=mesh,
        in_specs=(P("gz", "tile", None),) + (P(),) * 14,
        out_specs=P("gz", "tile", None),
        check_vma=False,
    )
```

```python
import numpy as np
import jax
import jax.numpy as jnp
from jax import lax
from jax.experimental import pallas as pl
from jax.experimental.pallas import tpu as pltpu
from jax.sharding import PartitionSpec as P


BF = jnp.bfloat16
F32 = jnp.float32
HALO = 8
GROUP = 8
GROUP5 = 6
LANES = 128
U_STACK, U_FIRST, U_SECOND, U_THIRD, U_FOURTH, U_FIFTH, U_SIXTH = 24, 22, 10, 8, 6, 5, 8
MATS = 13
CODE = 64


def up(n, m):
    return -(-n // m) * m


def starts(total, size):
    size = min(size, total)
    s = list(range(0, total - size + 1, size))
    if s[-1] + size < total:
        s.append(total - size)
    return size, s


def lanes_of(dims, row_of, rows2_of, x_of, width):
    zs, xs, cs = dims
    t = np.full((3, width), -1, np.int32)
    for z in range(zs):
        for x in range(xs):
            for i in range(cs):
                c = (z * xs + x) * cs + i
                t[0, c] = row_of(z, x, i)
                t[1, c] = rows2_of(z, x, i)
                t[2, c] = x_of(z, x, i)
    return t


class Plan:
    def __init__(self, zl, xl, ny, cf, cc):
        h = HALO
        self.zl, self.xl, self.ny, self.cf, self.cc = zl, xl, ny, cf, cc
        self.nh = ny // 2
        self.zd, self.xd = zl + 2 * h, xl + 2 * h
        self.z1, self.x1 = self.zd - 2, self.xd - 2
        self.z2, self.x2 = self.zd - 4, self.xd - 4
        self.zp, self.xp = self.z2 // 2, self.x2 // 2
        self.z3, self.x3 = self.zp - 2, self.xp - 2
        self.z4, self.x4 = self.zp - 4, self.xp - 4
        self.zs, self.xs = zl + 4, xl + 4
        self.z5, self.x5 = zl + 2, xl + 2
        self.sx = up(3 * self.xd, 16)
        self.k1 = up(3 * self.sx, 128)
        self.n2 = self.x2 // GROUP
        self.rest = self.x2 - self.n2 * GROUP
        self.g5, self.s5 = starts(self.x5, GROUP5)
        self.k2 = up(3 * (GROUP + 2) * cf, 128)
        self.kr = up(4 * (self.rest + 2) * cf, 128)
        self.k3 = up(3 * self.xp * cf, 128)
        self.k4 = up(3 * self.x3 * cc, 128)
        self.k5 = up(3 * (self.g5 + 2) * cf, 128)
        self.kc = up(2 * self.x4 * cc, 128)
        self.k6 = up(3 * self.x5 * cf, 128)
        self.cells = zl * xl
        self.span = 2 * LANES

    def tables(self):
        cf, cc = self.cf, self.cc
        none = lambda z, x, i: -1
        xof = lambda z, x, i: x
        code = lambda z, x, i: CODE * z + i
        a2 = lanes_of((3, GROUP + 2, cf), code, none, xof, self.k2)
        r0 = lanes_of((4, self.rest + 2, cf), lambda z, x, i: CODE * z + i if z < 3 else -1, none, xof, self.kr)
        r1 = lanes_of((4, self.rest + 2, cf), lambda z, x, i: CODE * (z - 1) + i if z else -1, none, xof, self.kr)
        a6 = lanes_of((3, self.x5, cf), code, none, xof, self.k6)
        a5 = lanes_of((3, self.g5 + 2, cf), code, none, xof, self.k5)
        ce = lanes_of(
            (2, self.x4, cc),
            lambda z, x, i: CODE * z + cf + i,
            lambda z, x, i: CODE * 2 + cf + i if z == 1 else -1,
            xof,
            self.kc,
        )
        co = lanes_of(
            (2, self.x4, cc),
            lambda z, x, i: CODE * 2 * z + cf + i,
            lambda z, x, i: CODE + cf + i if z == 0 else -1,
            xof,
            self.kc,
        )
        b4 = lanes_of((3, self.x3, cc), code, none, xof, self.k4)
        b3 = lanes_of((3, self.xp, cf), lambda z, x, i: 9 * cf * z + i, none, xof, self.k3)
        f1 = np.full((3, self.k1), -1, np.int32)
        for z in range(3):
            for dy in range(3):
                for x in range(self.xd):
                    c = z * self.sx + dy * self.xd + x
                    f1[0, c] = z * 24 + dy
                    f1[2, c] = x
        hd = lanes_of((1, self.cells, cf), lambda z, x, i: i, none, xof, self.cells * cf)
        return [a2, r0, r1, a6, a5, ce, co, b4, b3, f1, hd]


def prep_kernel(plan, widths, *refs):
    (tab, w2, w6, w5, w4, w3, w1, wh, bh) = refs[:9]
    biases = refs[9:15]
    (a1, a2, ar, a3, a4, a5, ac0, ac1, a6, hd, pm, pt, bias) = refs[15:28]
    (t1,) = refs[28:]
    p = plan
    cf, cc = p.cf, p.cc
    off = np.concatenate([[0], np.cumsum(widths)]).tolist()

    def dot(a, b):
        return jnp.dot(a, b, preferred_element_type=F32)

    def expand(w, i, j, co):
        lo, hi = off[i], off[j]
        rows = w.shape[1]
        r = lax.broadcasted_iota(jnp.int32, (rows, hi - lo), 0)
        total = None
        for dz in range(3):
            m = (r + CODE * dz == tab[0:1, lo:hi]) | (r + CODE * dz == tab[1:2, lo:hi])
            g = dot(w[dz * 9 * co : (dz + 1) * 9 * co, :], jnp.where(m, 1.0, 0.0).astype(BF))
            total = g if total is None else total + g
        return total

    def select(w, i, base):
        lo, hi = off[i], off[i + 1]
        r = lax.broadcasted_iota(jnp.int32, (w.shape[1], hi - lo), 0)
        m = (r - base == tab[0:1, lo:hi]) & (tab[0:1, lo:hi] >= 0)
        return dot(w, jnp.where(m, 1.0, 0.0).astype(BF))

    def band(pieces, i, pick, outs):
        xi = tab[2:3, off[i] : off[i + 1]]
        parts = []
        for xo in range(outs):
            acc = None
            for dx in range(3):
                v = jnp.where(xi == pick(xo, dx), pieces[dx], 0.0)
                acc = v if acc is None else acc + v
            parts.append(acc)
        return parts

    def rows_of(g, lo, width, dy, co):
        return [
            g[(dx * 3 + dy) * co : (dx * 3 + dy + 1) * co, lo : lo + width] for dx in range(3)
        ]

    def full(out, g, lo, i, pick, outs, co):
        parts = []
        for dy in range(3):
            parts += band(rows_of(g, lo, widths[i], dy, co), i, pick, outs)
        out[...] = jnp.concatenate(parts, axis=0).astype(BF)

    near = lambda xo, dx: xo + dx
    half = lambda xo, dx: (xo + dx) // 2
    t1[...] = jnp.zeros(t1.shape, F32)
    for k in range(9):
        t1[8 * k : 8 * k + 3, :cf] = w1[k // 3, k % 3].astype(F32)
    turned = t1[...].T[:cf].astype(BF)
    a1[...] = jnp.concatenate(
        band([select(turned, 9, 8 * dx) for dx in range(3)], 9, near, p.x1), axis=0
    ).astype(BF)
    g = expand(w2, 0, 3, cf)
    full(a2, g, 0, 0, near, GROUP, cf)
    parts = []
    for dy in range(3):
        for zo in range(2):
            lo = off[1 + zo]
            parts += band(rows_of(g, lo, p.kr, dy, cf), 1 + zo, near, p.rest)
    if parts:
        ar[...] = jnp.concatenate(parts, axis=0).astype(BF)
    full(a6, expand(w6, 3, 4, cf), 0, 3, near, p.xl, cf)
    g = expand(w5, 4, 7, cf)
    full(a5, g, 0, 4, near, p.g5, cf)
    full(ac0, g, off[5] - off[4], 5, half, p.x5, cf)
    full(ac1, g, off[6] - off[4], 6, half, p.x5, cf)
    full(a4, expand(w4, 7, 8, cc), 0, 7, near, p.x4, cc)
    turned = w3[...].astype(F32).T.astype(BF)
    parts = []
    for dy in range(3):
        pieces = [select(turned, 8, (3 * dx + dy) * cf) for dx in range(3)]
        parts += band(pieces, 8, near, p.x3)
    a3[...] = jnp.concatenate(parts, axis=0).astype(BF)
    v = select(jnp.broadcast_to(wh[...], (16, cf)), 10, 0)
    r = lax.broadcasted_iota(jnp.int32, (p.cells, p.cells * cf), 0)
    cell = tab[2:3, off[10] : off[11]]
    hd[...] = jnp.where(cell == r, v[0:1], 0.0).astype(BF)
    r = lax.broadcasted_iota(jnp.int32, (p.span, p.span), 0)
    c = lax.broadcasted_iota(jnp.int32, (p.span, p.span), 1)
    fold = lambda k: jnp.where(k < LANES, 2 * k, 2 * (k - LANES) + 1)
    pm[...] = jnp.where(r == fold(c), 1.0, 0.0).astype(BF)
    pt[...] = jnp.where(c == fold(r), 1.0, 0.0).astype(BF)
    at = 0
    for b in biases:
        n = b.shape[0]
        m = up(n, 8)
        r = lax.broadcasted_iota(jnp.int32, (m, p.nh), 0)
        v = jnp.zeros((m, p.nh), F32)
        for k in range(n):
            v = jnp.where(r == k, b[k], v)
        bias[at : at + m, :] = v
        at += m
    bias[at : at + 8, :] = jnp.broadcast_to(bh[...], (8, p.nh))


def repeat(n, unroll, body):
    unroll = max(u for u in range(1, unroll + 1) if n % u == 0)
    if unroll == n:
        for k in range(n):
            body(k)
        return

    def step(t, carry):
        for k in range(unroll):
            body(t * unroll + k)
        return carry

    lax.fori_loop(0, n // unroll, step, 0)


def main_kernel(plan, *refs):
    p = plan
    blocks = refs[:9]
    (a1, a2, ar, a3, a4, a5, ac0, ac1, a6, hd, pm, pt, bias) = refs[9 : 9 + MATS]
    out = refs[9 + MATS]
    (dd, se, so, m1, sk, po, c1, c2, de, rf) = refs[10 + MATS :]
    cf, cc, nh = p.cf, p.cc, p.nh

    def rows(lo, n):
        return bias[lo : lo + n, :]

    def dot(a, b):
        return jnp.dot(a, b, preferred_element_type=F32)

    def act(v, b, c):
        n = v.shape[0] // c
        u = v.reshape(n, c, nh) + b[None]
        return jnp.maximum(u, 0.1 * u).reshape(n * c, nh).astype(BF)

    def right(v):
        return pltpu.roll(v, 1, 1)

    def left(v):
        return pltpu.roll(v, nh - 1, 1)

    def window(ref, base, slab, rows, k, lo, slabs=3):
        parts = [
            ref[pl.ds(pl.multiple_of(base + dz * slab, 16), rows), lo : lo + nh]
            for dz in range(slabs)
        ]
        fill = k - slabs * rows
        while fill > 0:
            parts.append(parts[0][: min(fill, rows)])
            fill -= rows
        return jnp.concatenate(parts, axis=0)

    def taps(e, o, n):
        even = right(o[:n]) + e[n : 2 * n] + o[2 * n :]
        odd = e[:n] + o[n : 2 * n] + left(e[2 * n :])
        return even, odd

    h = HALO
    span = p.span
    raw = jnp.concatenate([b[...] for b in blocks], axis=0)
    split = [dot(raw[:, y : y + span], pm[...]) for y in range(0, p.ny, span)]
    row = 0
    for bz, nz in ((0, h), (h, p.zl), (h + p.zl, h)):
        for bx, nx in ((0, h), (h, p.xl), (h + p.xl, h)):
            for k, v in enumerate(split):
                v = v[row : row + nz * nx].reshape(nz, nx, span)
                at = slice(k * LANES, (k + 1) * LANES)
                dd[bz : bz + nz, bx : bx + nx, at] = v[:, :, :LANES]
                at = slice(nh + k * LANES, nh + (k + 1) * LANES)
                dd[bz : bz + nz, bx : bx + nx, at] = v[:, :, LANES:]
            row += nz * nx

    def stack(z):
        e = dd[z, :, :nh]
        o = dd[z, :, nh:]
        pad = jnp.zeros((p.sx - 3 * p.xd, nh), F32)
        at = pl.ds(pl.multiple_of(z * p.sx, 16), p.sx)
        se[at, :] = jnp.concatenate([right(o), e, o, pad], axis=0).astype(BF)
        so[at, :] = jnp.concatenate([e, o, left(e), pad], axis=0).astype(BF)

    repeat(p.zd, U_STACK, stack)
    tail = p.zd * p.sx
    se[tail:, :] = jnp.zeros((se.shape[0] - tail, nh), BF)
    so[tail:, :] = jnp.zeros((so.shape[0] - tail, nh), BF)

    r1 = p.x1 * cf
    b_first, b_second = rows(0, cf), rows(cf, cf)
    b_third, b_fourth = rows(2 * cf, cc), rows(2 * cf + cc, cc)
    b_fifth, b_sixth = rows(2 * cf + 2 * cc, cf), rows(3 * cf + 2 * cc, cf)

    def first(z):
        at = pl.ds(pl.multiple_of(z * p.sx, 16), p.k1)
        to = pl.ds(pl.multiple_of(z * r1, 16), r1)
        m1[to, :nh] = act(dot(a1[...], se[at, :]), b_first, cf)
        m1[to, nh:] = act(dot(a1[...], so[at, :]), b_first, cf)

    repeat(p.z1, U_FIRST, first)

    rp = p.xp * cf
    rs = p.xs * cf
    lead = (p.x2 - p.xs) // 2


    def keep(z, s, even, odd):
        lo, hi = max(s, lead), min(s + even.shape[0] // cf, lead + p.xs)
        if lo < hi:
            src = slice((lo - s) * cf, (hi - s) * cf)
            to = pl.ds(pl.multiple_of(z * rs + (lo - lead) * cf, 16), (hi - lo) * cf)
            sk[to, :nh] = even[src]
            sk[to, nh:] = odd[src]

    def pairs(even, odd):
        t = even.astype(F32) + odd.astype(F32)
        t = t.reshape(t.shape[0] // (2 * cf), 2, cf, nh)
        return t[:, 0] + t[:, 1]

    def pool(zz, s, total):
        n = total.shape[0] * cf
        pooled = (0.125 * total).reshape(n, nh).astype(BF)
        po[pl.ds(pl.multiple_of(zz * rp + s // 2 * cf, 16), n), :] = pooled

    def second(zz):
        for s in range(0, p.n2 * GROUP, GROUP):
            n = GROUP * cf
            total = None
            for dz in range(2):
                base = (2 * zz + dz) * r1 + s * cf
                k = (GROUP + 2) * cf
                e = dot(a2[...], window(m1, base, r1, k, p.k2, 0))
                o = dot(a2[...], window(m1, base, r1, k, p.k2, nh))
                even, odd = taps(e, o, n)
                even = act(even, b_second, cf)
                odd = act(odd, b_second, cf)
                keep(2 * zz + dz, s, even, odd)
                t = pairs(even, odd)
                total = t if total is None else total + t
            pool(zz, s, total)
        if p.rest:
            s = p.n2 * GROUP
            n = p.rest * cf
            base = 2 * zz * r1 + s * cf
            k = (p.rest + 2) * cf
            e = dot(ar[...], window(m1, base, r1, k, p.kr, 0, 4))
            o = dot(ar[...], window(m1, base, r1, k, p.kr, nh, 4))
            even, odd = taps(e, o, 2 * n)
            even = act(even, b_second, cf)
            odd = act(odd, b_second, cf)
            keep(2 * zz, s, even[:n], odd[:n])
            keep(2 * zz + 1, s, even[n:], odd[n:])
            t = pairs(even, odd)
            pool(zz, s, t[: p.rest // 2] + t[p.rest // 2 :])

    repeat(p.zp, U_SECOND, second)
    tail = p.zp * rp
    po[tail:, :] = jnp.zeros((po.shape[0] - tail, nh), BF)

    r3 = p.x3 * cc

    def third(z):
        v = dot(a3[...], po[pl.ds(pl.multiple_of(z * rp, 16), p.k3), :])
        v = right(v[:r3]) + v[r3 : 2 * r3] + left(v[2 * r3 :])
        c1[pl.ds(pl.multiple_of(z * r3, 16), r3), :] = act(v, b_third, cc)

    repeat(p.z3, U_THIRD, third)
    r4 = p.x4 * cc

    def fourth(z):
        v = dot(a4[...], window(c1, z * r3, r3, r3, p.k4, 0))
        v = right(v[:r4]) + v[r4 : 2 * r4] + left(v[2 * r4 :])
        c2[pl.ds(pl.multiple_of(z * r4, 16), r4), :] = act(v, b_fourth, cc)

    repeat(p.z4, U_FOURTH, fourth)
    tail = p.z4 * r4
    c2[tail:, :] = jnp.zeros((c2.shape[0] - tail, nh), BF)
    r5 = p.x5 * cf
    skip_lead = (p.z2 - p.zs) // 2

    def fifth(pair):
        for odd_z in range(2):
            z = 2 * pair + odd_z
            ac = ac0 if odd_z else ac1
            q = dot(ac[...], c2[pl.ds(pl.multiple_of(pair * r4, 16), p.kc), :])
            q0, q1, q2 = q[:r5], q[r5 : 2 * r5], q[2 * r5 :]
            done = 0
            e3 = [[], [], []]
            o3 = [[], [], []]
            n = p.g5 * cf
            for s in p.s5:
                rows = (p.g5 + 2) * cf
                base = (z + skip_lead) * rs + s * cf
                e = dot(a5[...], window(sk, base, rs, rows, p.k5, 0))
                o = dot(a5[...], window(sk, base, rs, rows, p.k5, nh))
                new = (done - s) * cf
                for dy in range(3):
                    e3[dy].append(e[dy * n + new : (dy + 1) * n])
                    o3[dy].append(o[dy * n + new : (dy + 1) * n])
                done = s + p.g5
            e0, e1, e2 = (jnp.concatenate(v, axis=0) for v in e3)
            o0, o1, o2 = (jnp.concatenate(v, axis=0) for v in o3)
            even = right(o0 + q0) + (e1 + o2 + (q1 + q2))
            odd = (e0 + o1 + (q0 + q1)) + left(e2 + q2)
            to = pl.ds(pl.multiple_of(z * r5, 16), r5)
            de[to, :nh] = act(even, b_fifth, cf)
            de[to, nh:] = act(odd, b_fifth, cf)

    repeat(p.z5 // 2, U_FIFTH, fifth)
    tail = p.z5 * r5
    de[tail:, :] = jnp.zeros((de.shape[0] - tail, p.ny), BF)
    r6 = p.xl * cf

    def sixth(z):
        at = pl.ds(pl.multiple_of(z * r5, 16), p.k6)
        e = dot(a6[...], de[at, :nh])
        o = dot(a6[...], de[at, nh:])
        even, odd = taps(e, o, r6)
        to = pl.ds(pl.multiple_of(z * r6, 16), r6)
        rf[to, :nh] = act(even, b_sixth, cf)
        rf[to, nh:] = act(odd, b_sixth, cf)

    repeat(p.zl, U_SIXTH, sixth)
    last = 4 * cf + 2 * cc
    field = dot(hd[...], rf[...]) + bias[last : last + 1, 0:1]
    high = field.astype(BF)
    low = (field - high.astype(F32)).astype(BF)
    both = jnp.concatenate([high, low], axis=0)
    for k in range(p.ny // span):
        at = slice(k * LANES, (k + 1) * LANES)
        v = jnp.concatenate([both[:, at], both[:, nh + k * LANES : nh + (k + 1) * LANES]], axis=1)
        v = dot(v, pt[...])
        out[:, k * span : (k + 1) * span] = v[: p.cells] + v[p.cells :]


def shift(block, axis, step):
    count = lax.axis_size(axis)
    return lax.ppermute(block, axis, [((i + step) % count, i) for i in range(count)])


def body(
    density,
    w_first,
    b_first,
    w_second,
    b_second,
    w_third,
    b_third,
    w_fourth,
    b_fourth,
    w_fifth,
    b_fifth,
    w_sixth,
    b_sixth,
    w_head,
    b_head,
):
    zl, xl, ny = density.shape
    cf, cc = w_second.shape[0], w_third.shape[0]
    h = HALO
    p = Plan(zl, xl, ny, cf, cc)

    left = shift(density[:, xl - h :], "tile", -1)
    right = shift(density[:, :h], "tile", 1)
    columns = [left, density, right]
    below = [shift(c[zl - h :], "gz", -1) for c in columns]
    above = [shift(c[:h], "gz", 1) for c in columns]
    blocks = [b.reshape(-1, ny) for b in below + columns + above]

    def taps(w, *last):
        return w.transpose(2, 3, 4, *last).reshape(-1, w.shape[last[1]])

    weights = [taps(w, 0, 1) for w in (w_second, w_sixth, w_fifth, w_fourth)]
    weights += [taps(w_third, 1, 0), w_first[:, 0].transpose(1, 2, 3, 0), w_head[None], b_head[None]]
    biases = [b_first, b_second, b_third, b_fourth, b_fifth, b_sixth]
    tabs = p.tables()
    widths = [t.shape[1] for t in tabs]
    tab = jnp.asarray(np.concatenate(tabs, axis=1))
    bias_rows = sum(up(b.shape[0], 8) for b in biases + [b_head])

    mats = [
        pltpu.VMEM((p.x1 * cf, p.k1), BF),
        pltpu.VMEM((3 * GROUP * cf, p.k2), BF),
        pltpu.VMEM((max(6 * p.rest * cf, 16), p.kr), BF),
        pltpu.VMEM((3 * p.x3 * cc, p.k3), BF),
        pltpu.VMEM((3 * p.x4 * cc, p.k4), BF),
        pltpu.VMEM((3 * p.g5 * cf, p.k5), BF),
        pltpu.VMEM((3 * p.x5 * cf, p.kc), BF),
        pltpu.VMEM((3 * p.x5 * cf, p.kc), BF),
        pltpu.VMEM((3 * p.xl * cf, p.k6), BF),
        pltpu.VMEM((p.cells, p.cells * cf), BF),
        pltpu.VMEM((p.span, p.span), BF),
        pltpu.VMEM((p.span, p.span), BF),
        pltpu.VMEM((bias_rows, p.nh), F32),
    ]
    vmem = pl.BlockSpec(memory_space=pltpu.VMEM)
    smem = pl.BlockSpec(memory_space=pltpu.SMEM)
    tables = pl.pallas_call(
        lambda *refs: prep_kernel(p, widths, *refs),
        in_specs=[vmem] * 9 + [smem] * 6,
        out_specs=[vmem] * MATS,
        out_shape=mats,
        scratch_shapes=[pltpu.VMEM((72, LANES), F32)],
        name="bands",
    )(tab, *weights, *biases)

    def on_chip(arrays):
        return [pltpu.with_memory_space_constraint(v, pltpu.VMEM) for v in arrays]

    field = pl.pallas_call(
        lambda *refs: main_kernel(p, *refs),
        in_specs=[vmem] * (9 + MATS),
        out_specs=vmem,
        out_shape=jax.ShapeDtypeStruct((p.cells, ny), F32),
        scratch_shapes=[
            pltpu.VMEM((p.zd, p.xd, ny), F32),
            pltpu.VMEM((p.zd * p.sx + 256, p.nh), BF),
            pltpu.VMEM((p.zd * p.sx + 256, p.nh), BF),
            pltpu.VMEM((p.z1 * p.x1 * cf, ny), BF),
            pltpu.VMEM((p.z2 * p.xs * cf, ny), BF),
            pltpu.VMEM((p.zp * p.xp * cf + 256, p.nh), BF),
            pltpu.VMEM((p.z3 * p.x3 * cc, p.nh), BF),
            pltpu.VMEM((p.z4 * p.x4 * cc + 256, p.nh), BF),
            pltpu.VMEM((p.z5 * p.x5 * cf + 256, ny), BF),
            pltpu.VMEM((p.cells * cf, ny), BF),
        ],
        name="unet",
    )(*on_chip(blocks), *on_chip(tables))
    return field.reshape(zl, xl, ny)


def solution(mesh):
    return jax.shard_map(
        body,
        mesh=mesh,
        in_specs=(P("gz", "tile", None),) + (P(),) * 14,
        out_specs=P("gz", "tile", None),
        check_vma=False,
    )
```

```python
import numpy as np
import jax
import jax.numpy as jnp
from jax import lax
from jax.experimental import pallas as pl
from jax.experimental.pallas import tpu as pltpu
from jax.sharding import PartitionSpec as P


BF = jnp.bfloat16
F32 = jnp.float32
HALO = 8
GROUP = 8
GROUP5 = 6
GROUP4 = 3
LANES = 128
MATS = 13
VMEM_LIMIT = 52 << 20
CODE = 64


def up(n, m):
    return -(-n // m) * m


def starts(total, size, step):
    size = min(size, total)
    assert (total - size) % step == 0
    s = list(range(0, total - size + 1, size))
    if s[-1] + size < total:
        s.append(total - size)
    return size, s


def lanes_of(dims, row_of, rows2_of, x_of, width):
    zs, xs, cs = dims
    t = np.full((3, width), -1, np.int32)
    for z in range(zs):
        for x in range(xs):
            for i in range(cs):
                c = (z * xs + x) * cs + i
                t[0, c] = row_of(z, x, i)
                t[1, c] = rows2_of(z, x, i)
                t[2, c] = x_of(z, x, i)
    return t


class Plan:
    def __init__(self, zl, xl, ny, cf, cc):
        h = HALO
        self.zl, self.xl, self.ny, self.cf, self.cc = zl, xl, ny, cf, cc
        self.nh = ny // 2
        self.zd, self.xd = zl + 2 * h, xl + 2 * h
        self.z1, self.x1 = self.zd - 2, self.xd - 2
        self.z2, self.x2 = self.zd - 4, self.xd - 4
        self.zp, self.xp = self.z2 // 2, self.x2 // 2
        self.z3, self.x3 = self.zp - 2, self.xp - 2
        self.z4, self.x4 = self.zp - 4, self.xp - 4
        self.zs, self.xs = zl + 4, xl + 4
        self.z5, self.x5 = zl + 2, xl + 2
        self.sx = up(3 * self.xd, 16)
        self.k1 = up(3 * self.sx, 128)
        self.n2 = self.x2 // GROUP
        self.rest = self.x2 - self.n2 * GROUP
        self.g4, self.s4 = starts(self.x4, GROUP4, 1)
        self.g5, self.s5 = starts(self.x5, GROUP5, 2)
        self.k2 = up(3 * (GROUP + 2) * cf, 128)
        self.kr = up(4 * (self.rest + 2) * cf, 128)
        self.k3 = up(3 * self.xp * cf, 128)
        self.k4 = up(3 * (self.g4 + 2) * cc, 128)
        self.k5 = up(3 * (self.g5 + 2) * cf, 128)
        self.kc = up(2 * self.x4 * cc, 128)
        self.k6 = up(3 * self.x5 * cf, 128)
        self.cells = zl * xl
        self.span = 2 * LANES

    def tables(self):
        cf, cc = self.cf, self.cc
        none = lambda z, x, i: -1
        xof = lambda z, x, i: x
        code = lambda z, x, i: CODE * z + i
        a2 = lanes_of((3, GROUP + 2, cf), code, none, xof, self.k2)
        r0 = lanes_of((4, self.rest + 2, cf), lambda z, x, i: CODE * z + i if z < 3 else -1, none, xof, self.kr)
        r1 = lanes_of((4, self.rest + 2, cf), lambda z, x, i: CODE * (z - 1) + i if z else -1, none, xof, self.kr)
        a6 = lanes_of((3, self.x5, cf), code, none, xof, self.k6)
        a5 = lanes_of((3, self.g5 + 2, cf), code, none, xof, self.k5)
        ce = lanes_of(
            (2, self.x4, cc),
            lambda z, x, i: CODE * z + cf + i,
            lambda z, x, i: CODE * 2 + cf + i if z == 1 else -1,
            xof,
            self.kc,
        )
        co = lanes_of(
            (2, self.x4, cc),
            lambda z, x, i: CODE * 2 * z + cf + i,
            lambda z, x, i: CODE + cf + i if z == 0 else -1,
            xof,
            self.kc,
        )
        b4 = lanes_of((3, self.g4 + 2, cc), code, none, xof, self.k4)
        b3 = lanes_of((3, self.xp, cf), lambda z, x, i: cf * z + i, none, xof, self.k3)
        f1 = np.full((3, self.k1), -1, np.int32)
        for z in range(3):
            for dy in range(3):
                for x in range(self.xd):
                    c = z * self.sx + dy * self.xd + x
                    f1[0, c] = z * 24 + dy
                    f1[2, c] = x
        hd = lanes_of((1, self.cells, cf), lambda z, x, i: i, none, xof, self.cells * cf)
        return [a2, r0, r1, a6, a5, ce, co, b4, b3, f1, hd]


def prep_kernel(plan, widths, *refs):
    (tab, w2, w6, w5, w4, w3, w1, wh) = refs[:8]
    biases = refs[8:14]
    block = refs[14]
    (a1, a2, ar, a3, a4, a5, ac0, ac1, a6, hd, pm, pt, bias) = refs[15 : 15 + MATS]
    own, t1, t3 = refs[15 + MATS :]
    own[...] = block[...]
    p = plan
    cf, cc = p.cf, p.cc
    off = np.concatenate([[0], np.cumsum(widths)]).tolist()

    def expand(w, i, j, co):
        lo, hi = off[i], off[j]
        rows = w.shape[1]
        r = lax.broadcasted_iota(jnp.int32, (rows, hi - lo), 0)
        total = None
        for dz in range(3):
            m = (r + CODE * dz == tab[0:1, lo:hi]) | (r + CODE * dz == tab[1:2, lo:hi])
            g = dot(w[dz * 9 * co : (dz + 1) * 9 * co, :], jnp.where(m, 1.0, 0.0).astype(BF))
            total = g if total is None else total + g
        return total

    def select(w, i, base):
        lo, hi = off[i], off[i + 1]
        r = lax.broadcasted_iota(jnp.int32, (w.shape[1], hi - lo), 0)
        m = (r - base == tab[0:1, lo:hi]) & (tab[0:1, lo:hi] >= 0)
        return dot(w, jnp.where(m, 1.0, 0.0).astype(BF))

    def band(pieces, i, pick, outs):
        xi = tab[2:3, off[i] : off[i + 1]]
        parts = []
        for xo in range(outs):
            sums = {}
            for dx in range(3):
                at = pick(xo, dx)
                sums[at] = sums[at] + pieces[dx] if at in sums else pieces[dx]
            v = 0.0
            for at, piece in sums.items():
                v = jnp.where(xi == at, piece, v)
            parts.append(v)
        return parts

    def rows_of(g, lo, width, dy, co):
        return [
            g[(dx * 3 + dy) * co : (dx * 3 + dy + 1) * co, lo : lo + width] for dx in range(3)
        ]

    def full(out, g, lo, i, pick, outs, co):
        parts = []
        for dy in range(3):
            parts += band(rows_of(g, lo, widths[i], dy, co), i, pick, outs)
        out[...] = jnp.concatenate(parts, axis=0).astype(BF)

    near = lambda xo, dx: xo + dx
    half = lambda xo, dx: (xo + dx) // 2
    t1[...] = jnp.zeros(t1.shape, F32)
    for k in range(9):
        t1[8 * k : 8 * k + 3, :cf] = w1[k // 3, k % 3].astype(F32)
    turned = t1[...].T[:cf].astype(BF)
    a1[...] = jnp.concatenate(
        band([select(turned, 9, 8 * dx) for dx in range(3)], 9, near, p.x1), axis=0
    ).astype(BF)
    g = expand(w2, 0, 3, cf)
    full(a2, g, 0, 0, near, GROUP, cf)
    parts = []
    for dy in range(3):
        for zo in range(2):
            lo = off[1 + zo]
            parts += band(rows_of(g, lo, p.kr, dy, cf), 1 + zo, near, p.rest)
    if parts:
        ar[...] = jnp.concatenate(parts, axis=0).astype(BF)
    full(a6, expand(w6, 3, 4, cf), 0, 3, near, p.xl, cf)
    g = expand(w5, 4, 7, cf)
    full(a5, g, 0, 4, near, p.g5, cf)
    full(ac0, g, off[5] - off[4], 5, half, p.x5, cf)
    full(ac1, g, off[6] - off[4], 6, half, p.x5, cf)
    full(a4, expand(w4, 7, 8, cc), 0, 7, near, p.g4, cc)
    t3[...] = jnp.zeros(t3.shape, F32)
    for k in range(27):
        dz, j = k // 9, k % 9
        t3[dz * cf : (dz + 1) * cf, j * cc : (j + 1) * cc] = w3[
            k * cf : (k + 1) * cf, :
        ].astype(F32)
    turned = t3[...].T[: 9 * cc].astype(BF)
    full(a3, select(turned, 8, 0), 0, 8, near, p.x3, cc)
    v = select(jnp.broadcast_to(wh[...], (16, cf)), 10, 0)
    r = lax.broadcasted_iota(jnp.int32, (p.cells, p.cells * cf), 0)
    cell = tab[2:3, off[10] : off[11]]
    hd[...] = jnp.where(cell == r, v[0:1], 0.0).astype(BF)
    fold = lambda k: jnp.where(k < LANES, 2 * k, 2 * (k - LANES) + 1)
    r = lax.broadcasted_iota(jnp.int32, (p.span, p.span), 0)
    c = lax.broadcasted_iota(jnp.int32, (1, p.span), 1)
    pm[...] = jnp.where(r == fold(c), 1.0, 0.0).astype(BF)
    r = fold(lax.broadcasted_iota(jnp.int32, (p.span, LANES), 0))
    c = lax.broadcasted_iota(jnp.int32, (p.span, LANES), 1)
    pt[...] = jnp.where(jnp.concatenate([r - c, r - c - LANES], axis=1) == 0, 1.0, 0.0).astype(BF)
    at = 0
    for b in biases:
        n = b.shape[0]
        m = up(n, 8)
        r = lax.broadcasted_iota(jnp.int32, (m, p.nh), 0)
        v = jnp.zeros((m, p.nh), F32)
        for k in range(n):
            v = jnp.where(r == k, b[k], v)
        bias[at : at + m, :] = v
        at += m


def dot(a, b):
    return jnp.dot(a, b, preferred_element_type=F32)


def right(v):
    return pltpu.roll(v, 1, 1)


def left(v):
    return pltpu.roll(v, v.shape[1] - 1, 1)


def act(v, b):
    c = b.shape[0]
    u = v.reshape(v.shape[0] // c, c, v.shape[1]) + b[None]
    return jnp.maximum(u, 0.1 * u).reshape(v.shape).astype(BF)


def taps(e, o, n):
    even = right(o[:n]) + e[n : 2 * n] + o[2 * n :]
    odd = e[:n] + o[n : 2 * n] + left(e[2 * n :])
    return even, odd


def window(slabs, off, rows, k, cols):
    parts = [ref[base + off : base + off + rows, cols] for ref, base in slabs]
    fill = k - len(slabs) * rows
    while fill > 0:
        parts.append(parts[0][: min(fill, rows)])
        fill -= rows
    return jnp.concatenate(parts, axis=0)


def bias_rows(p, bias):
    cf, cc = p.cf, p.cc
    sizes = [cf, cf, cc, cc, cf, cf]
    at = np.concatenate([[0], np.cumsum([up(n, 8) for n in sizes])]).tolist()
    return [bias[lo : lo + n, :] for lo, n in zip(at, sizes)]


def runs(zs):
    out = []
    for z in zs:
        if out and out[-1][1] == z:
            out[-1][1] = z + 1
        else:
            out.append([z, z + 1])
    return out


def front(p, mats, blocks, dd, se, so, zs, m1, sk, po):
    a1, a2, ar, pm, b_first, b_second = mats
    cf, nh, span = p.cf, p.nh, p.span
    even_y, odd_y = slice(0, nh), slice(nh, None)
    pieces, places = [], []
    for ref, z0, x0, nx in blocks:
        nz = ref.shape[0] // nx
        for lo, hi in runs([z for z in zs if z0 <= z < z0 + nz]):
            pieces.append(ref[(lo - z0) * nx : (hi - z0) * nx, :])
            places.append((lo, hi, x0, nx))
    raw = jnp.concatenate(pieces, axis=0)
    split = [dot(raw[:, y : y + span], pm[...]) for y in range(0, p.ny, span)]
    row = 0
    for lo, hi, x0, nx in places:
        n = (hi - lo) * nx
        for k, v in enumerate(split):
            v = v[row : row + n].reshape(hi - lo, nx, span)
            for at, src in ((k * LANES, slice(0, LANES)), (nh + k * LANES, slice(LANES, None))):
                dd[lo:hi, x0 : x0 + nx, at : at + LANES] = v[:, :, src]
        row += n
    for z in zs:
        e = dd[z, :, even_y]
        o = dd[z, :, odd_y]
        pad = jnp.zeros((p.sx - 3 * p.xd, nh), F32)
        at = slice(z * p.sx, (z + 1) * p.sx)
        se[at, :] = jnp.concatenate([right(o), e, o, pad], axis=0).astype(BF)
        so[at, :] = jnp.concatenate([e, o, left(e), pad], axis=0).astype(BF)
    tail = p.k1 - 3 * p.sx
    for _, z in runs(zs):
        se[z * p.sx : z * p.sx + tail, :] = jnp.zeros((tail, nh), BF)
        so[z * p.sx : z * p.sx + tail, :] = jnp.zeros((tail, nh), BF)

    r1 = p.x1 * cf
    for z in [z for z in zs if z + 1 in zs and z + 2 in zs]:
        at = slice(z * p.sx, z * p.sx + p.k1)
        ref, to = m1[z]
        ref[to : to + r1, even_y] = act(dot(a1[...], se[at, :]), b_first)
        ref[to : to + r1, odd_y] = act(dot(a1[...], so[at, :]), b_first)

    lead = (p.x2 - p.xs) // 2

    def keep(z, s, even, odd):
        lo, hi = max(s, lead), min(s + even.shape[0] // cf, lead + p.xs)
        if lo < hi and z in sk:
            src = slice((lo - s) * cf, (hi - s) * cf)
            ref, base = sk[z]
            to = slice(base + (lo - lead) * cf, base + (hi - lead) * cf)
            ref[to, even_y] = even[src]
            ref[to, odd_y] = odd[src]

    def pairs(even, odd):
        t = even.astype(F32) + odd.astype(F32)
        t = t.reshape(t.shape[0] // (2 * cf), 2, cf, nh)
        return t[:, 0] + t[:, 1]

    def pool(zz, s, total):
        n = total.shape[0] * cf
        ref, base = po[zz]
        to = base + s // 2 * cf
        ref[to : to + n, :] = (0.125 * total).reshape(n, nh).astype(BF)

    for zz in sorted(po):
        slabs = [m1[2 * zz + k] for k in range(4)]
        for s in range(0, p.n2 * GROUP, GROUP):
            total = None
            rows = (GROUP + 2) * cf
            for dz in range(2):
                e = dot(a2[...], window(slabs[dz : dz + 3], s * cf, rows, p.k2, even_y))
                o = dot(a2[...], window(slabs[dz : dz + 3], s * cf, rows, p.k2, odd_y))
                even, odd = taps(e, o, GROUP * cf)
                even, odd = act(even, b_second), act(odd, b_second)
                keep(2 * zz + dz, s, even, odd)
                t = pairs(even, odd)
                total = t if total is None else total + t
            pool(zz, s, total)
        if p.rest:
            s = p.n2 * GROUP
            n = p.rest * cf
            rows = (p.rest + 2) * cf
            e = dot(ar[...], window(slabs, s * cf, rows, p.kr, even_y))
            o = dot(ar[...], window(slabs, s * cf, rows, p.kr, odd_y))
            even, odd = taps(e, o, 2 * n)
            even, odd = act(even, b_second), act(odd, b_second)
            keep(2 * zz, s, even[:n], odd[:n])
            keep(2 * zz + 1, s, even[n:], odd[n:])
            t = pairs(even, odd)
            pool(zz, s, t[: p.rest // 2] + t[p.rest // 2 :])


def early_kernel(plan, *refs):
    p = plan
    h = HALO
    (b0, b1, b2, a1, a2, ar, pm, bias, bh, mu, ku, pu, last, dd, se, so) = refs
    last[...] = jnp.full(last.shape, bh[0], F32)
    b_first, b_second = bias_rows(p, bias)[:2]
    xs = ((0, h), (h, p.xl), (h + p.xl, h))
    blocks = [(b, h, x, n) for b, (x, n) in zip((b0, b1, b2), xs)]
    r1, rs, rp = p.x1 * p.cf, p.xs * p.cf, p.xp * p.cf
    m1 = {h + k: (mu, k * r1) for k in range(p.zl - 2)}
    sk = {h + k: (ku, k * rs) for k in range(p.zl - 4)}
    po = {h // 2 + k: (pu, k * rp) for k in range(p.zl // 2 - 2)}
    zs = list(range(h, h + p.zl))
    front(p, (a1, a2, ar, pm, b_first, b_second), blocks, dd, se, so, zs, m1, sk, po)


def main_kernel(plan, *refs):
    p = plan
    blocks = refs[:9]
    (a1, a2, ar, a3, a4, a5, ac0, ac1, a6, hd, pm, pt, bias) = refs[9 : 9 + MATS]
    mu, ku, pu, last, out = refs[9 + MATS : 14 + MATS]
    (dd, se, so, m1, sk, po, c1, c2, de, rf) = refs[14 + MATS :]
    cf, cc, nh = p.cf, p.cc, p.nh
    h = HALO
    even_y, odd_y = slice(0, nh), slice(nh, None)
    b_first, b_second, b_third, b_fourth, b_fifth, b_sixth = bias_rows(p, bias)

    ways = lambda n: ((0, h), (h, n), (h + n, h))
    placed = [
        (blocks[3 * i + j], z, x, nx)
        for i, (z, _) in enumerate(ways(p.zl))
        for j, (x, nx) in enumerate(ways(p.xl))
    ]
    r1, rs, rp = p.x1 * cf, p.xs * cf, p.xp * cf
    lead = (p.z2 - p.zs) // 2
    done1 = range(h, h + p.zl - 2)
    done2 = range(h, h + p.zl - 4)
    donep = range(h // 2, h // 2 + p.zl // 2 - 2)
    first_at = {z: (mu, (z - h) * r1) if z in done1 else (m1, z * r1) for z in range(p.z1)}
    skip_at = {
        z: (ku, (z - h) * rs) if z in done2 else (sk, (z - lead) * rs)
        for z in range(lead, lead + p.zs)
    }
    pool_at = {
        z: (pu, (z - h // 2) * rp) if z in donep else (po, z * rp) for z in range(p.zp)
    }
    below = list(range(h + 2))
    above = list(range(h + p.zl - 2, p.zd))
    front(
        p,
        (a1, a2, ar, pm, b_first, b_second),
        placed,
        dd,
        se,
        so,
        below + above,
        first_at,
        skip_at,
        {z: v for z, v in pool_at.items() if z not in donep},
    )

    r3 = p.x3 * cc
    for z in range(p.z3):
        v = dot(a3[...], window([pool_at[z + k] for k in range(3)], 0, rp, p.k3, even_y))
        v = right(v[:r3]) + v[r3 : 2 * r3] + left(v[2 * r3 :])
        c1[z * r3 : (z + 1) * r3, :] = act(v, b_third)
    r4 = p.x4 * cc
    n4 = p.g4 * cc
    for z in range(p.z4):
        slabs = [(c1, (z + k) * r3) for k in range(3)]
        for s in p.s4:
            v = dot(a4[...], window(slabs, s * cc, n4 + 2 * cc, p.k4, even_y))
            v = right(v[:n4]) + v[n4 : 2 * n4] + left(v[2 * n4 :])
            to = z * r4 + s * cc
            c2[to : to + n4, :] = act(v, b_fourth)
    tail = p.z4 * r4
    c2[tail:, :] = jnp.zeros((c2.shape[0] - tail, nh), BF)

    r5 = p.x5 * cf
    for z in range(p.z5):
        ac = ac0 if z % 2 else ac1
        at = z // 2 * r4
        q = dot(ac[...], c2[at : at + p.kc, :])
        q0, q1, q2 = q[:r5], q[r5 : 2 * r5], q[2 * r5 :]
        slabs = [skip_at[z + lead + k] for k in range(3)]
        done = 0
        e3 = [[], [], []]
        o3 = [[], [], []]
        n = p.g5 * cf
        rows = (p.g5 + 2) * cf
        for s in p.s5:
            e = dot(a5[...], window(slabs, s * cf, rows, p.k5, even_y))
            o = dot(a5[...], window(slabs, s * cf, rows, p.k5, odd_y))
            new = (done - s) * cf
            for dy in range(3):
                e3[dy].append(e[dy * n + new : (dy + 1) * n])
                o3[dy].append(o[dy * n + new : (dy + 1) * n])
            done = s + p.g5
        e0, e1, e2 = (jnp.concatenate(v, axis=0) for v in e3)
        o0, o1, o2 = (jnp.concatenate(v, axis=0) for v in o3)
        even = right(o0 + q0) + (e1 + o2 + (q1 + q2))
        odd = (e0 + o1 + (q0 + q1)) + left(e2 + q2)
        de[z * r5 : (z + 1) * r5, even_y] = act(even, b_fifth)
        de[z * r5 : (z + 1) * r5, odd_y] = act(odd, b_fifth)
    tail = p.z5 * r5
    de[tail:, :] = jnp.zeros((de.shape[0] - tail, p.ny), BF)

    r6 = p.xl * cf
    for z in range(p.zl):
        at = slice(z * r5, z * r5 + p.k6)
        even, odd = taps(dot(a6[...], de[at, even_y]), dot(a6[...], de[at, odd_y]), r6)
        rf[z * r6 : (z + 1) * r6, even_y] = act(even, b_sixth)
        rf[z * r6 : (z + 1) * r6, odd_y] = act(odd, b_sixth)
    field = dot(hd[...], rf[...]) + last[0:1, 0:1]
    high = field.astype(BF)
    low = (field - high.astype(F32)).astype(BF)
    both = jnp.concatenate([high, low], axis=0)
    for k in range(p.ny // p.span):
        at = slice(k * LANES, (k + 1) * LANES)
        v = jnp.concatenate([both[:, at], both[:, nh + k * LANES : nh + (k + 1) * LANES]], axis=1)
        v = dot(v, pt[...])
        out[:, k * p.span : (k + 1) * p.span] = v[: p.cells] + v[p.cells :]


def shift(block, axis, step):
    count = lax.axis_size(axis)
    return lax.ppermute(block, axis, [((i + step) % count, i) for i in range(count)])


def body(
    density,
    w_first,
    b_first,
    w_second,
    b_second,
    w_third,
    b_third,
    w_fourth,
    b_fourth,
    w_fifth,
    b_fifth,
    w_sixth,
    b_sixth,
    w_head,
    b_head,
):
    zl, xl, ny = density.shape
    cf, cc = w_second.shape[0], w_third.shape[0]
    h = HALO
    p = Plan(zl, xl, ny, cf, cc)

    prev = shift(density[:, xl - h :], "tile", -1)
    after = shift(density[:, :h], "tile", 1)
    columns = [prev, density, after]
    below, above = [], []
    for c in columns:
        below.append(shift(c[zl - h :], "gz", -1))
        above.append(shift(c[:h], "gz", 1))
    below, columns, above = (
        [b.reshape(-1, ny) for b in row] for row in (below, columns, above)
    )

    def by_tap(w, *last):
        return w.transpose(2, 3, 4, *last).reshape(-1, w.shape[last[1]])

    weights = [by_tap(w, 0, 1) for w in (w_second, w_sixth, w_fifth, w_fourth)]
    weights += [by_tap(w_third, 1, 0), w_first[:, 0].transpose(1, 2, 3, 0), w_head[None]]
    biases = [b_first, b_second, b_third, b_fourth, b_fifth, b_sixth]
    tabs = p.tables()
    widths = [t.shape[1] for t in tabs]
    tab = jnp.asarray(np.concatenate(tabs, axis=1))
    bias_count = sum(up(b.shape[0], 8) for b in biases)

    mats = [
        pltpu.VMEM((p.x1 * cf, p.k1), BF),
        pltpu.VMEM((3 * GROUP * cf, p.k2), BF),
        pltpu.VMEM((max(6 * p.rest * cf, 16), p.kr), BF),
        pltpu.VMEM((3 * p.x3 * cc, p.k3), BF),
        pltpu.VMEM((3 * p.g4 * cc, p.k4), BF),
        pltpu.VMEM((3 * p.g5 * cf, p.k5), BF),
        pltpu.VMEM((3 * p.x5 * cf, p.kc), BF),
        pltpu.VMEM((3 * p.x5 * cf, p.kc), BF),
        pltpu.VMEM((3 * p.xl * cf, p.k6), BF),
        pltpu.VMEM((p.cells, p.cells * cf), BF),
        pltpu.VMEM((p.span, p.span), BF),
        pltpu.VMEM((p.span, p.span), BF),
        pltpu.VMEM((bias_count, p.nh), F32),
    ]
    vmem = pl.BlockSpec(memory_space=pltpu.VMEM)
    smem = pl.BlockSpec(memory_space=pltpu.SMEM)
    room = pltpu.CompilerParams(vmem_limit_bytes=VMEM_LIMIT)

    def in_hbm(arrays):
        return [pltpu.with_memory_space_constraint(v, pltpu.HBM) for v in arrays]

    *tables, own = pl.pallas_call(
        lambda *refs: prep_kernel(p, widths, *refs),
        in_specs=[vmem] * 8 + [smem] * 6 + [vmem],
        out_specs=[vmem] * (MATS + 1),
        out_shape=mats + [pltpu.VMEM((zl * xl, ny), BF)],
        scratch_shapes=[pltpu.VMEM((72, LANES), F32), pltpu.VMEM((LANES, up(9 * cc, LANES)), F32)],
        name="bands",
    )(*in_hbm([tab] + weights), *biases, *in_hbm([columns[1]]))
    columns[1] = own

    def on_chip(arrays):
        return [pltpu.with_memory_space_constraint(v, pltpu.VMEM) for v in arrays]

    stacks = [
        pltpu.VMEM((p.zd, p.xd, ny), F32),
        pltpu.VMEM((p.zd * p.sx + 256, p.nh), BF),
        pltpu.VMEM((p.zd * p.sx + 256, p.nh), BF),
    ]
    ready = pl.pallas_call(
        lambda *refs: early_kernel(p, *refs),
        in_specs=[vmem] * 8 + [smem],
        out_specs=[vmem] * 4,
        out_shape=[
            pltpu.VMEM(((zl - 2) * p.x1 * cf, ny), BF),
            pltpu.VMEM(((zl - 4) * p.xs * cf, ny), BF),
            pltpu.VMEM(((zl // 2 - 2) * p.xp * cf, p.nh), BF),
            pltpu.VMEM((8, LANES), F32),
        ],
        scratch_shapes=stacks,
        compiler_params=room,
        name="early",
    )(*on_chip(columns), *on_chip([tables[k] for k in (0, 1, 2, 10, 12)]), b_head)

    field = pl.pallas_call(
        lambda *refs: main_kernel(p, *refs),
        in_specs=[vmem] * (9 + MATS + 4),
        out_specs=vmem,
        out_shape=jax.ShapeDtypeStruct((p.cells, ny), F32),
        scratch_shapes=stacks
        + [
            pltpu.VMEM((p.z1 * p.x1 * cf, ny), BF),
            pltpu.VMEM((p.zs * p.xs * cf, ny), BF),
            pltpu.VMEM((p.zp * p.xp * cf, p.nh), BF),
            pltpu.VMEM((p.z3 * p.x3 * cc, p.nh), BF),
            pltpu.VMEM((p.z4 * p.x4 * cc + 256, p.nh), BF),
            pltpu.VMEM((p.z5 * p.x5 * cf + 256, ny), BF),
            pltpu.VMEM((p.cells * cf, ny), BF),
        ],
        compiler_params=room,
        name="unet",
    )(*on_chip(below + columns + above), *on_chip(tables), *on_chip(ready))
    return field.reshape(zl, xl, ny)


def solution(mesh):
    return jax.shard_map(
        body,
        mesh=mesh,
        in_specs=(P("gz", "tile", None),) + (P(),) * 14,
        out_specs=P("gz", "tile", None),
        check_vma=False,
    )
```

```python
import numpy as np
import jax
import jax.numpy as jnp
from jax import lax
from jax.experimental import pallas as pl
from jax.experimental.pallas import tpu as pltpu
from jax.sharding import PartitionSpec as P


BF = jnp.bfloat16
F32 = jnp.float32
HALO = 8
GROUP = 8
GROUP5 = 6
GROUP4 = 3
LANES = 128
MATS = 13
VMEM_LIMIT = 52 << 20
CODE = 64


def up(n, m):
    return -(-n // m) * m


def starts(total, size, step):
    size = min(size, total)
    assert (total - size) % step == 0
    s = list(range(0, total - size + 1, size))
    if s[-1] + size < total:
        s.append(total - size)
    return size, s


def lanes_of(dims, row_of, rows2_of, x_of, width):
    zs, xs, cs = dims
    t = np.full((3, width), -1, np.int32)
    for z in range(zs):
        for x in range(xs):
            for i in range(cs):
                c = (z * xs + x) * cs + i
                t[0, c] = row_of(z, x, i)
                t[1, c] = rows2_of(z, x, i)
                t[2, c] = x_of(z, x, i)
    return t


class Plan:
    def __init__(self, zl, xl, ny, cf, cc):
        h = HALO
        self.zl, self.xl, self.ny, self.cf, self.cc = zl, xl, ny, cf, cc
        self.nh = ny // 2
        self.zd, self.xd = zl + 2 * h, xl + 2 * h
        self.z1, self.x1 = self.zd - 2, self.xd - 2
        self.z2, self.x2 = self.zd - 4, self.xd - 4
        self.zp, self.xp = self.z2 // 2, self.x2 // 2
        self.z3, self.x3 = self.zp - 2, self.xp - 2
        self.z4, self.x4 = self.zp - 4, self.xp - 4
        self.zs, self.xs = zl + 4, xl + 4
        self.z5, self.x5 = zl + 2, xl + 2
        self.sx = up(3 * self.xd, 16)
        self.k1 = up(3 * self.sx, 128)
        self.n2 = self.x2 // GROUP
        self.rest = self.x2 - self.n2 * GROUP
        self.g4, self.s4 = starts(self.x4, GROUP4, 1)
        self.g5, self.s5 = starts(self.x5, GROUP5, 2)
        self.k2 = up(3 * (GROUP + 2) * cf, 128)
        self.kr = up(4 * (self.rest + 2) * cf, 128)
        self.k3 = up(3 * self.xp * cf, 128)
        self.k4 = up(3 * (self.g4 + 2) * cc, 128)
        self.k5 = up(3 * (self.g5 + 2) * cf, 128)
        self.kc = up(2 * self.x4 * cc, 128)
        self.k6 = up(3 * self.x5 * cf, 128)
        self.cells = zl * xl
        self.span = 2 * LANES

    def tables(self):
        cf, cc = self.cf, self.cc
        none = lambda z, x, i: -1
        xof = lambda z, x, i: x
        code = lambda z, x, i: CODE * z + i
        a2 = lanes_of((3, GROUP + 2, cf), code, none, xof, self.k2)
        r0 = lanes_of((4, self.rest + 2, cf), lambda z, x, i: CODE * z + i if z < 3 else -1, none, xof, self.kr)
        r1 = lanes_of((4, self.rest + 2, cf), lambda z, x, i: CODE * (z - 1) + i if z else -1, none, xof, self.kr)
        a6 = lanes_of((3, self.x5, cf), code, none, xof, self.k6)
        a5 = lanes_of((3, self.g5 + 2, cf), code, none, xof, self.k5)
        ce = lanes_of(
            (2, self.x4, cc),
            lambda z, x, i: CODE * z + cf + i,
            lambda z, x, i: CODE * 2 + cf + i if z == 1 else -1,
            xof,
            self.kc,
        )
        co = lanes_of(
            (2, self.x4, cc),
            lambda z, x, i: CODE * 2 * z + cf + i,
            lambda z, x, i: CODE + cf + i if z == 0 else -1,
            xof,
            self.kc,
        )
        b4 = lanes_of((3, self.g4 + 2, cc), code, none, xof, self.k4)
        b3 = lanes_of((3, self.xp, cf), lambda z, x, i: cf * z + i, none, xof, self.k3)
        f1 = np.full((3, self.k1), -1, np.int32)
        for z in range(3):
            for dy in range(3):
                for x in range(self.xd):
                    c = z * self.sx + dy * self.xd + x
                    f1[0, c] = z * 24 + dy
                    f1[2, c] = x
        hd = lanes_of((1, self.cells, cf), lambda z, x, i: i, none, xof, self.cells * cf)
        return [a2, r0, r1, a6, a5, ce, co, b4, b3, f1, hd]


def prep_kernel(plan, widths, *refs):
    (tab, w2, w6, w5, w4, w3, w1, wh) = refs[:8]
    biases = refs[8:14]
    block = refs[14]
    (a1, a2, ar, a3, a4, a5, ac0, ac1, a6, hd, pm, pt, bias) = refs[15 : 15 + MATS]
    own, t1, t3 = refs[15 + MATS :]
    own[...] = block[...]
    p = plan
    cf, cc = p.cf, p.cc
    off = np.concatenate([[0], np.cumsum(widths)]).tolist()

    def expand(w, i, j, co):
        lo, hi = off[i], off[j]
        rows = w.shape[1]
        r = lax.broadcasted_iota(jnp.int32, (rows, hi - lo), 0)
        total = None
        for dz in range(3):
            m = (r + CODE * dz == tab[0:1, lo:hi]) | (r + CODE * dz == tab[1:2, lo:hi])
            g = dot(w[dz * 9 * co : (dz + 1) * 9 * co, :], jnp.where(m, 1.0, 0.0).astype(BF))
            total = g if total is None else total + g
        return total

    def select(w, i, base):
        lo, hi = off[i], off[i + 1]
        r = lax.broadcasted_iota(jnp.int32, (w.shape[1], hi - lo), 0)
        m = (r - base == tab[0:1, lo:hi]) & (tab[0:1, lo:hi] >= 0)
        return dot(w, jnp.where(m, 1.0, 0.0).astype(BF))

    def band(pieces, i, pick, outs):
        xi = tab[2:3, off[i] : off[i + 1]]
        parts = []
        for xo in range(outs):
            sums = {}
            for dx in range(3):
                at = pick(xo, dx)
                sums[at] = sums[at] + pieces[dx] if at in sums else pieces[dx]
            v = 0.0
            for at, piece in sums.items():
                v = jnp.where(xi == at, piece, v)
            parts.append(v)
        return parts

    def rows_of(g, lo, width, dy, co):
        return [
            g[(dx * 3 + dy) * co : (dx * 3 + dy + 1) * co, lo : lo + width] for dx in range(3)
        ]

    def full(out, g, lo, i, pick, outs, co):
        parts = []
        for dy in range(3):
            parts += band(rows_of(g, lo, widths[i], dy, co), i, pick, outs)
        out[...] = jnp.concatenate(parts, axis=0).astype(BF)

    near = lambda xo, dx: xo + dx
    half = lambda xo, dx: (xo + dx) // 2
    t1[...] = jnp.zeros(t1.shape, F32)
    for k in range(9):
        t1[8 * k : 8 * k + 3, :cf] = w1[k // 3, k % 3].astype(F32)
    turned = t1[...].T[:cf].astype(BF)
    a1[...] = jnp.concatenate(
        band([select(turned, 9, 8 * dx) for dx in range(3)], 9, near, p.x1), axis=0
    ).astype(BF)
    g = expand(w2, 0, 3, cf)
    full(a2, g, 0, 0, near, GROUP, cf)
    parts = []
    for dy in range(3):
        for zo in range(2):
            lo = off[1 + zo]
            parts += band(rows_of(g, lo, p.kr, dy, cf), 1 + zo, near, p.rest)
    if parts:
        ar[...] = jnp.concatenate(parts, axis=0).astype(BF)
    full(a6, expand(w6, 3, 4, cf), 0, 3, near, p.xl, cf)
    g = expand(w5, 4, 7, cf)
    full(a5, g, 0, 4, near, p.g5, cf)
    full(ac0, g, off[5] - off[4], 5, half, p.x5, cf)
    full(ac1, g, off[6] - off[4], 6, half, p.x5, cf)
    full(a4, expand(w4, 7, 8, cc), 0, 7, near, p.g4, cc)
    t3[...] = jnp.zeros(t3.shape, F32)
    for k in range(27):
        dz, j = k // 9, k % 9
        t3[dz * cf : (dz + 1) * cf, j * cc : (j + 1) * cc] = w3[
            k * cf : (k + 1) * cf, :
        ].astype(F32)
    turned = t3[...].T[: 9 * cc].astype(BF)
    full(a3, select(turned, 8, 0), 0, 8, near, p.x3, cc)
    v = select(jnp.broadcast_to(wh[...], (16, cf)), 10, 0)
    r = lax.broadcasted_iota(jnp.int32, (p.cells, p.cells * cf), 0)
    cell = tab[2:3, off[10] : off[11]]
    hd[...] = jnp.where(cell == r, v[0:1], 0.0).astype(BF)
    fold = lambda k: jnp.where(k < LANES, 2 * k, 2 * (k - LANES) + 1)
    r = lax.broadcasted_iota(jnp.int32, (p.span, p.span), 0)
    c = lax.broadcasted_iota(jnp.int32, (1, p.span), 1)
    pm[...] = jnp.where(r == fold(c), 1.0, 0.0).astype(BF)
    r = fold(lax.broadcasted_iota(jnp.int32, (p.span, LANES), 0))
    c = lax.broadcasted_iota(jnp.int32, (p.span, LANES), 1)
    pt[...] = jnp.where(jnp.concatenate([r - c, r - c - LANES], axis=1) == 0, 1.0, 0.0).astype(BF)
    at = 0
    for b in biases:
        n = b.shape[0]
        m = up(n, 8)
        r = lax.broadcasted_iota(jnp.int32, (m, p.nh), 0)
        v = jnp.zeros((m, p.nh), F32)
        for k in range(n):
            v = jnp.where(r == k, b[k], v)
        bias[at : at + m, :] = v
        at += m


def dot(a, b):
    return jnp.dot(a, b, preferred_element_type=F32)


def right(v):
    return pltpu.roll(v, 1, 1)


def left(v):
    return pltpu.roll(v, v.shape[1] - 1, 1)


def act(v, b):
    c = b.shape[0]
    u = v.reshape(v.shape[0] // c, c, v.shape[1]) + b[None]
    return jnp.maximum(u, 0.1 * u).reshape(v.shape).astype(BF)


def taps(e, o, n):
    even = right(o[:n]) + e[n : 2 * n] + o[2 * n :]
    odd = e[:n] + o[n : 2 * n] + left(e[2 * n :])
    return even, odd


def window(slabs, off, rows, k, cols):
    parts = [ref[base + off : base + off + rows, cols] for ref, base in slabs]
    fill = k - len(slabs) * rows
    while fill > 0:
        parts.append(parts[0][: min(fill, rows)])
        fill -= rows
    return jnp.concatenate(parts, axis=0)


def bias_rows(p, bias):
    cf, cc = p.cf, p.cc
    sizes = [cf, cf, cc, cc, cf, cf]
    at = np.concatenate([[0], np.cumsum([up(n, 8) for n in sizes])]).tolist()
    return [bias[lo : lo + n, :] for lo, n in zip(at, sizes)]


def runs(zs):
    out = []
    for z in zs:
        if out and out[-1][1] == z:
            out[-1][1] = z + 1
        else:
            out.append([z, z + 1])
    return out


def front(p, mats, blocks, dd, se, so, zs, m1, sk, po):
    a1, a2, ar, pm, b_first, b_second = mats
    cf, nh, span = p.cf, p.nh, p.span
    even_y, odd_y = slice(0, nh), slice(nh, None)
    for first_z, end_z in runs(zs):
        pieces, places = [], []
        for ref, z0, x0, nx in blocks:
            lo, hi = max(z0, first_z), min(z0 + ref.shape[0] // nx, end_z)
            if lo < hi:
                pieces.append(ref[(lo - z0) * nx : (hi - z0) * nx, :])
                places.append((lo, hi, x0, nx))
        raw = jnp.concatenate(pieces, axis=0)
        split = [dot(raw[:, y : y + span], pm[...]) for y in range(0, p.ny, span)]
        row = 0
        for lo, hi, x0, nx in places:
            n = (hi - lo) * nx
            for k, v in enumerate(split):
                v = v[row : row + n].reshape(hi - lo, nx, span)
                for at, src in ((k * LANES, slice(0, LANES)), (nh + k * LANES, slice(LANES, None))):
                    dd[lo:hi, x0 : x0 + nx, at : at + LANES] = v[:, :, src]
            row += n
        for z in range(first_z, end_z):
            e = dd[z, :, even_y]
            o = dd[z, :, odd_y]
            pad = jnp.zeros((p.sx - 3 * p.xd, nh), F32)
            at = slice(z * p.sx, (z + 1) * p.sx)
            se[at, :] = jnp.concatenate([right(o), e, o, pad], axis=0).astype(BF)
            so[at, :] = jnp.concatenate([e, o, left(e), pad], axis=0).astype(BF)
    tail = p.k1 - 3 * p.sx
    for _, z in runs(zs):
        se[z * p.sx : z * p.sx + tail, :] = jnp.zeros((tail, nh), BF)
        so[z * p.sx : z * p.sx + tail, :] = jnp.zeros((tail, nh), BF)

    r1 = p.x1 * cf
    for z in [z for z in zs if z + 1 in zs and z + 2 in zs]:
        at = slice(z * p.sx, z * p.sx + p.k1)
        ref, to = m1[z]
        ref[to : to + r1, even_y] = act(dot(a1[...], se[at, :]), b_first)
        ref[to : to + r1, odd_y] = act(dot(a1[...], so[at, :]), b_first)

    lead = (p.x2 - p.xs) // 2

    def keep(z, s, even, odd):
        lo, hi = max(s, lead), min(s + even.shape[0] // cf, lead + p.xs)
        if lo < hi and z in sk:
            src = slice((lo - s) * cf, (hi - s) * cf)
            ref, base = sk[z]
            to = slice(base + (lo - lead) * cf, base + (hi - lead) * cf)
            ref[to, even_y] = even[src]
            ref[to, odd_y] = odd[src]

    def pairs(even, odd):
        t = even.astype(F32) + odd.astype(F32)
        t = t.reshape(t.shape[0] // (2 * cf), 2, cf, nh)
        return t[:, 0] + t[:, 1]

    def pool(zz, s, total):
        n = total.shape[0] * cf
        ref, base = po[zz]
        to = base + s // 2 * cf
        ref[to : to + n, :] = (0.125 * total).reshape(n, nh).astype(BF)

    for zz in sorted(po):
        slabs = [m1[2 * zz + k] for k in range(4)]
        for s in range(0, p.n2 * GROUP, GROUP):
            total = None
            rows = (GROUP + 2) * cf
            for dz in range(2):
                e = dot(a2[...], window(slabs[dz : dz + 3], s * cf, rows, p.k2, even_y))
                o = dot(a2[...], window(slabs[dz : dz + 3], s * cf, rows, p.k2, odd_y))
                even, odd = taps(e, o, GROUP * cf)
                even, odd = act(even, b_second), act(odd, b_second)
                keep(2 * zz + dz, s, even, odd)
                t = pairs(even, odd)
                total = t if total is None else total + t
            pool(zz, s, total)
        if p.rest:
            s = p.n2 * GROUP
            n = p.rest * cf
            rows = (p.rest + 2) * cf
            e = dot(ar[...], window(slabs, s * cf, rows, p.kr, even_y))
            o = dot(ar[...], window(slabs, s * cf, rows, p.kr, odd_y))
            even, odd = taps(e, o, 2 * n)
            even, odd = act(even, b_second), act(odd, b_second)
            keep(2 * zz, s, even[:n], odd[:n])
            keep(2 * zz + 1, s, even[n:], odd[n:])
            t = pairs(even, odd)
            pool(zz, s, t[: p.rest // 2] + t[p.rest // 2 :])


def offset_kernel(value, out):
    out[...] = jnp.full(out.shape, value[0], F32)


def early_kernel(plan, *refs):
    p = plan
    h = HALO
    (b0, b1, b2, a1, a2, ar, pm, bias, mu, ku, pu, dd, se, so) = refs
    b_first, b_second = bias_rows(p, bias)[:2]
    xs = ((0, h), (h, p.xl), (h + p.xl, h))
    blocks = [(b, h, x, n) for b, (x, n) in zip((b0, b1, b2), xs)]
    r1, rs, rp = p.x1 * p.cf, p.xs * p.cf, p.xp * p.cf
    m1 = {h + k: (mu, k * r1) for k in range(p.zl - 2)}
    sk = {h + k: (ku, k * rs) for k in range(p.zl - 4)}
    po = {h // 2 + k: (pu, k * rp) for k in range(p.zl // 2 - 2)}
    zs = list(range(h, h + p.zl))
    front(p, (a1, a2, ar, pm, b_first, b_second), blocks, dd, se, so, zs, m1, sk, po)


def main_kernel(plan, *refs):
    p = plan
    blocks = refs[:9]
    (a1, a2, ar, a3, a4, a5, ac0, ac1, a6, hd, pm, pt, bias) = refs[9 : 9 + MATS]
    mu, ku, pu, last, out = refs[9 + MATS : 14 + MATS]
    (dd, se, so, m1, sk, po, c1, c2, de, rf) = refs[14 + MATS :]
    cf, cc, nh = p.cf, p.cc, p.nh
    h = HALO
    even_y, odd_y = slice(0, nh), slice(nh, None)
    b_first, b_second, b_third, b_fourth, b_fifth, b_sixth = bias_rows(p, bias)

    ways = lambda n: ((0, h), (h, n), (h + n, h))
    placed = [
        (blocks[3 * i + j], z, x, nx)
        for i, (z, _) in enumerate(ways(p.zl))
        for j, (x, nx) in enumerate(ways(p.xl))
    ]
    r1, rs, rp = p.x1 * cf, p.xs * cf, p.xp * cf
    lead = (p.z2 - p.zs) // 2
    done1 = range(h, h + p.zl - 2)
    done2 = range(h, h + p.zl - 4)
    donep = range(h // 2, h // 2 + p.zl // 2 - 2)
    first_at = {z: (mu, (z - h) * r1) if z in done1 else (m1, z * r1) for z in range(p.z1)}
    skip_at = {
        z: (ku, (z - h) * rs) if z in done2 else (sk, (z - lead) * rs)
        for z in range(lead, lead + p.zs)
    }
    pool_at = {
        z: (pu, (z - h // 2) * rp) if z in donep else (po, z * rp) for z in range(p.zp)
    }
    below = list(range(h + 2))
    above = list(range(h + p.zl - 2, p.zd))
    front(
        p,
        (a1, a2, ar, pm, b_first, b_second),
        placed,
        dd,
        se,
        so,
        below + above,
        first_at,
        skip_at,
        {z: v for z, v in pool_at.items() if z not in donep},
    )

    r3 = p.x3 * cc
    for z in range(p.z3):
        v = dot(a3[...], window([pool_at[z + k] for k in range(3)], 0, rp, p.k3, even_y))
        v = right(v[:r3]) + v[r3 : 2 * r3] + left(v[2 * r3 :])
        c1[z * r3 : (z + 1) * r3, :] = act(v, b_third)
    r4 = p.x4 * cc
    n4 = p.g4 * cc
    for z in range(p.z4):
        slabs = [(c1, (z + k) * r3) for k in range(3)]
        for s in p.s4:
            v = dot(a4[...], window(slabs, s * cc, n4 + 2 * cc, p.k4, even_y))
            v = right(v[:n4]) + v[n4 : 2 * n4] + left(v[2 * n4 :])
            to = z * r4 + s * cc
            c2[to : to + n4, :] = act(v, b_fourth)
    tail = p.z4 * r4
    c2[tail:, :] = jnp.zeros((c2.shape[0] - tail, nh), BF)

    r5 = p.x5 * cf
    for z in range(p.z5):
        ac = ac0 if z % 2 else ac1
        at = z // 2 * r4
        q = dot(ac[...], c2[at : at + p.kc, :])
        q0, q1, q2 = q[:r5], q[r5 : 2 * r5], q[2 * r5 :]
        slabs = [skip_at[z + lead + k] for k in range(3)]
        done = 0
        e3 = [[], [], []]
        o3 = [[], [], []]
        n = p.g5 * cf
        rows = (p.g5 + 2) * cf
        for s in p.s5:
            e = dot(a5[...], window(slabs, s * cf, rows, p.k5, even_y))
            o = dot(a5[...], window(slabs, s * cf, rows, p.k5, odd_y))
            new = (done - s) * cf
            for dy in range(3):
                e3[dy].append(e[dy * n + new : (dy + 1) * n])
                o3[dy].append(o[dy * n + new : (dy + 1) * n])
            done = s + p.g5
        e0, e1, e2 = (jnp.concatenate(v, axis=0) for v in e3)
        o0, o1, o2 = (jnp.concatenate(v, axis=0) for v in o3)
        even = right(o0 + q0) + (e1 + o2 + (q1 + q2))
        odd = (e0 + o1 + (q0 + q1)) + left(e2 + q2)
        de[z * r5 : (z + 1) * r5, even_y] = act(even, b_fifth)
        de[z * r5 : (z + 1) * r5, odd_y] = act(odd, b_fifth)
    tail = p.z5 * r5
    de[tail:, :] = jnp.zeros((de.shape[0] - tail, p.ny), BF)

    r6 = p.xl * cf
    for z in range(p.zl):
        at = slice(z * r5, z * r5 + p.k6)
        even, odd = taps(dot(a6[...], de[at, even_y]), dot(a6[...], de[at, odd_y]), r6)
        rf[z * r6 : (z + 1) * r6, even_y] = act(even, b_sixth)
        rf[z * r6 : (z + 1) * r6, odd_y] = act(odd, b_sixth)
    field = dot(hd[...], rf[...]) + last[0:1, 0:1]
    high = field.astype(BF)
    low = (field - high.astype(F32)).astype(BF)
    both = jnp.concatenate([high, low], axis=0)
    for k in range(p.ny // p.span):
        at = slice(k * LANES, (k + 1) * LANES)
        v = jnp.concatenate([both[:, at], both[:, nh + k * LANES : nh + (k + 1) * LANES]], axis=1)
        v = dot(v, pt[...])
        out[:, k * p.span : (k + 1) * p.span] = v[: p.cells] + v[p.cells :]


def shift(block, axis, step):
    count = lax.axis_size(axis)
    return lax.ppermute(block, axis, [((i + step) % count, i) for i in range(count)])


def body(
    density,
    w_first,
    b_first,
    w_second,
    b_second,
    w_third,
    b_third,
    w_fourth,
    b_fourth,
    w_fifth,
    b_fifth,
    w_sixth,
    b_sixth,
    w_head,
    b_head,
):
    zl, xl, ny = density.shape
    cf, cc = w_second.shape[0], w_third.shape[0]
    h = HALO
    p = Plan(zl, xl, ny, cf, cc)

    prev = shift(density[:, xl - h :], "tile", -1)
    after = shift(density[:, :h], "tile", 1)
    columns = [prev, density, after]
    below, above = [], []
    for c in columns:
        below.append(shift(c[zl - h :], "gz", -1))
        above.append(shift(c[:h], "gz", 1))
    below, columns, above = (
        [b.reshape(-1, ny) for b in row] for row in (below, columns, above)
    )

    def by_tap(w, *last):
        return w.transpose(2, 3, 4, *last).reshape(-1, w.shape[last[1]])

    weights = [by_tap(w, 0, 1) for w in (w_second, w_sixth, w_fifth, w_fourth)]
    weights += [by_tap(w_third, 1, 0), w_first[:, 0].transpose(1, 2, 3, 0), w_head[None]]
    biases = [b_first, b_second, b_third, b_fourth, b_fifth, b_sixth]
    tabs = p.tables()
    widths = [t.shape[1] for t in tabs]
    tab = jnp.asarray(np.concatenate(tabs, axis=1))
    bias_count = sum(up(b.shape[0], 8) for b in biases)

    mats = [
        pltpu.VMEM((p.x1 * cf, p.k1), BF),
        pltpu.VMEM((3 * GROUP * cf, p.k2), BF),
        pltpu.VMEM((max(6 * p.rest * cf, 16), p.kr), BF),
        pltpu.VMEM((3 * p.x3 * cc, p.k3), BF),
        pltpu.VMEM((3 * p.g4 * cc, p.k4), BF),
        pltpu.VMEM((3 * p.g5 * cf, p.k5), BF),
        pltpu.VMEM((3 * p.x5 * cf, p.kc), BF),
        pltpu.VMEM((3 * p.x5 * cf, p.kc), BF),
        pltpu.VMEM((3 * p.xl * cf, p.k6), BF),
        pltpu.VMEM((p.cells, p.cells * cf), BF),
        pltpu.VMEM((p.span, p.span), BF),
        pltpu.VMEM((p.span, p.span), BF),
        pltpu.VMEM((bias_count, p.nh), F32),
    ]
    vmem = pl.BlockSpec(memory_space=pltpu.VMEM)
    smem = pl.BlockSpec(memory_space=pltpu.SMEM)
    room = pltpu.CompilerParams(vmem_limit_bytes=VMEM_LIMIT)

    def in_hbm(arrays):
        return [pltpu.with_memory_space_constraint(v, pltpu.HBM) for v in arrays]

    *tables, own = pl.pallas_call(
        lambda *refs: prep_kernel(p, widths, *refs),
        in_specs=[vmem] * 8 + [smem] * 6 + [vmem],
        out_specs=[vmem] * (MATS + 1),
        out_shape=mats + [pltpu.VMEM((zl * xl, ny), BF)],
        scratch_shapes=[pltpu.VMEM((72, LANES), F32), pltpu.VMEM((LANES, up(9 * cc, LANES)), F32)],
        name="bands",
    )(*in_hbm([tab] + weights), *biases, *in_hbm([columns[1]]))
    columns[1] = own

    def on_chip(arrays):
        return [pltpu.with_memory_space_constraint(v, pltpu.VMEM) for v in arrays]

    last = pl.pallas_call(
        offset_kernel,
        in_specs=[smem],
        out_specs=vmem,
        out_shape=pltpu.VMEM((8, LANES), F32),
        name="offset",
    )(b_head)

    stacks = [
        pltpu.VMEM((p.zd, p.xd, ny), F32),
        pltpu.VMEM((p.zd * p.sx + 256, p.nh), BF),
        pltpu.VMEM((p.zd * p.sx + 256, p.nh), BF),
    ]
    ready = pl.pallas_call(
        lambda *refs: early_kernel(p, *refs),
        in_specs=[vmem] * 8,
        out_specs=[vmem] * 3,
        out_shape=[
            pltpu.VMEM(((zl - 2) * p.x1 * cf, ny), BF),
            pltpu.VMEM(((zl - 4) * p.xs * cf, ny), BF),
            pltpu.VMEM(((zl // 2 - 2) * p.xp * cf, p.nh), BF),
        ],
        scratch_shapes=stacks,
        compiler_params=room,
        name="early",
    )(*on_chip(columns), *on_chip([tables[k] for k in (0, 1, 2, 10, 12)]))

    field = pl.pallas_call(
        lambda *refs: main_kernel(p, *refs),
        in_specs=[vmem] * (9 + MATS + 4),
        out_specs=vmem,
        out_shape=jax.ShapeDtypeStruct((p.cells, ny), F32),
        scratch_shapes=stacks
        + [
            pltpu.VMEM((p.z1 * p.x1 * cf, ny), BF),
            pltpu.VMEM((p.zs * p.xs * cf, ny), BF),
            pltpu.VMEM((p.zp * p.xp * cf, p.nh), BF),
            pltpu.VMEM((p.z3 * p.x3 * cc, p.nh), BF),
            pltpu.VMEM((p.z4 * p.x4 * cc + 256, p.nh), BF),
            pltpu.VMEM((p.z5 * p.x5 * cf + 256, ny), BF),
            pltpu.VMEM((p.cells * cf, ny), BF),
        ],
        compiler_params=room,
        name="unet",
    )(*on_chip(below + columns + above), *on_chip(tables), *on_chip(list(ready) + [last]))
    return field.reshape(zl, xl, ny)


def solution(mesh):
    return jax.shard_map(
        body,
        mesh=mesh,
        in_specs=(P("gz", "tile", None),) + (P(),) * 14,
        out_specs=P("gz", "tile", None),
        check_vma=False,
    )
```
